32 devices in a mesh: angle: 2 (over y), ty: 8 (over z, core), tx: 2 (over x).
Axes of the slice: x: 2, y: 2, z: 4, core: 2. Of those that a mesh axis runs over, the one named last changes fastest.
Arguments:
- object_slices: float32 [2, 2, 2048, 2048], P('angle', None, 'ty', 'tx'), may hold values from -5 to 5
- probe_field: float32 [2, 256, 256], replicated, may hold values from -6 to 6
- positions: int32 [2, 8, 2, 4, 2], P('angle', 'ty', 'tx'), may hold values from 0 to 1792, as said below
- live_slots: int32 [2, 8, 2], P('angle', 'ty', 'tx'), may hold values from 1 to 4, as said below
- photon_counts: int32 [2, 8, 2, 4, 256, 256], P('angle', 'ty', 'tx'), may hold values from 1 to 1600
Outputs:
- new_object: float32 [2, 2, 2048, 2048], P('angle', None, 'ty', 'tx')
- new_probe: float32 [2, 256, 256], P(None, 'ty')
The draws below stay inside these ranges and needn't reach their ends.
Inputs may be any that keep to these rules, and one draw needn't show every extreme that they name: `positions`: A slot's patch lies inside the object and its centre (top-left plus 128) lies in the rows and columns of the tile that holds the slot: rows r * 256 to (r + 1) * 256 - 1, columns c * 1024 to (c + 1) * 1024 - 1. `live_slots`: some tile of every draw uses all 4 slots.
All inputs are finite; a program needn't handle non-finite values.
Results may differ from the reference program's by a relative error of at most 0.0003.
Values sent between devices are 32-bit elements; how exact they have to be, the bound alone decides.
A program may use at most 128 MiB of HBM per device.

```python
import jax
import jax.numpy as jnp
from jax import lax

P_SIZE = 256
TR = 256
TC = 1024
SLOTS = 4
ANGLES = 2
NR = 2048
NC = 2048
N_TY = 8
N_TX = 2


def draw_positions(key, part):
    shape = (ANGLES, N_TY, N_TX, SLOTS)
    first_key, second_key = jax.random.split(jax.random.fold_in(key, 11))
    row_draw = jax.random.randint(first_key, shape, 0, TR)
    col_draw = jax.random.randint(second_key, shape, 0, TC)
    tile_row = lax.broadcasted_iota(jnp.int32, shape, 1)
    tile_col = lax.broadcasted_iota(jnp.int32, shape, 2)
    row_start = jnp.clip(tile_row * TR - P_SIZE // 2 + row_draw, 0, NR - P_SIZE)
    col_start = jnp.clip(tile_col * TC - P_SIZE // 2 + col_draw, 0, NC - P_SIZE)
    return jnp.stack([row_start, col_start], axis=-1).astype(jnp.int32)


def draw_live_slots(key, part):
    shape = (ANGLES, N_TY, N_TX)
    first_key, second_key, third_key = jax.random.split(jax.random.fold_in(key, 23), 3)
    sparse = jax.random.randint(first_key, shape, 1, max(SLOTS // 4, 1) + 1)
    dense = jax.random.randint(second_key, shape, 0, 8) == 0
    values = jnp.where(dense, SLOTS, sparse).reshape(-1)
    chosen = jax.random.randint(third_key, (), 0, ANGLES * N_TY * N_TX)
    values = jnp.where(jnp.arange(ANGLES * N_TY * N_TX) == chosen, SLOTS, values)
    return values.reshape(shape).astype(jnp.int32)


def set_ends(result, own_key, smallest, high):
    longest = result.shape.index(max(result.shape))
    spots = []
    for shift in (0, 1):
        where = [jax.random.randint(jax.random.fold_in(own_key, axis), (), 0, length) for axis, length in enumerate(result.shape)]
        where[longest] = (where[longest] + shift) % result.shape[longest]
        spots.append(tuple(where))
    return result.at[spots[0]].set(smallest).at[spots[1]].set(high)


def block_scale(stream_key, shape, cuts, smallest, largest):
    level, own = 1.0, jax.random.fold_in(stream_key, 6)
    for axis_at, parts in cuts:
        draws = jnp.exp(jax.random.uniform(jax.random.fold_in(own, axis_at), (parts,), jnp.float32, smallest / len(cuts), largest / len(cuts)))
        level = level * jnp.repeat(draws, shape[axis_at] // parts).reshape([-1 if axis == axis_at else 1 for axis in range(len(shape))])
    return level


def noise(stream_key, extent, width, limit, pieces=(), kind=jnp.bfloat16):
    gain = block_scale(stream_key, extent, pieces, -0.22, 0.18) if pieces else 1.0
    values = jax.random.normal(stream_key, extent, jnp.float32) * width * gain
    return jnp.minimum(jnp.maximum(values, -limit), limit).astype(kind)


def setup_inputs(seed: int = 0) -> dict:
    key_of = jax.random.split(jax.random.key(seed), 6)
    object_slices = noise(key_of[0], (ANGLES, 2, NR, NC), 0.7, 5.0, ((0, 2), (2, 8), (3, 2)), jnp.float32)
    probe_field = noise(key_of[1], (2, P_SIZE, P_SIZE), 1.0, 6.0, (), jnp.float32)
    positions = draw_positions(jax.random.fold_in(key_of[5], 71), 0)
    live_slots = draw_live_slots(jax.random.fold_in(key_of[5], 71), 0)
    photon_counts = set_ends(jax.random.randint(key_of[4], (ANGLES, N_TY, N_TX, SLOTS, P_SIZE, P_SIZE), 1, 1601), jax.random.fold_in(key_of[4], 1), 1, 1600).astype(jnp.int32)
    return {"object_slices": object_slices, "probe_field": probe_field, "positions": positions, "live_slots": live_slots, "photon_counts": photon_counts}


def reference(object_slices, probe_field, positions, live_slots, photon_counts):
    ftype = object_slices.dtype
    probe_wave = lax.complex(probe_field[0], probe_field[1])
    probe_power = probe_field[0] * probe_field[0] + probe_field[1] * probe_field[1]
    slot_index = jnp.arange(SLOTS, dtype=jnp.int32)
    probe_num = jnp.zeros((P_SIZE, P_SIZE), probe_wave.dtype)
    probe_den = jnp.zeros((P_SIZE, P_SIZE), ftype)
    numerators = []
    denominators = []
    fields = []
    for angle_index in range(ANGLES):
        field = lax.complex(object_slices[angle_index, 0], object_slices[angle_index, 1])
        spots = positions[angle_index].reshape(-1, 2).astype(jnp.int32)
        weights = (slot_index[None, None, :] < live_slots[angle_index][:, :, None]).astype(ftype).reshape(-1)
        measured = photon_counts[angle_index].reshape(-1, P_SIZE, P_SIZE)

        def deposit(carry, item):
            obj_num, obj_den, pr_num, pr_den = carry
            spot, weight, count = item
            row_at = spot[0].astype(jnp.int32)
            col_at = spot[1].astype(jnp.int32)
            patch = lax.dynamic_slice(field, (row_at, col_at), (P_SIZE, P_SIZE))
            wave = probe_wave * patch
            far = jnp.fft.fft2(wave, norm='ortho')
            amplitude = 0.05 * jnp.sqrt(count.astype(ftype))
            factor = amplitude * lax.rsqrt(jnp.maximum(far.real * far.real + far.imag * far.imag, 0.0625))
            gap = (jnp.fft.ifft2(far * factor, norm='ortho') - wave) * weight
            current = lax.dynamic_slice(obj_num, (row_at, col_at), (P_SIZE, P_SIZE))
            obj_num = lax.dynamic_update_slice(obj_num, current + jnp.conj(probe_wave) * gap, (row_at, col_at))
            current_den = lax.dynamic_slice(obj_den, (row_at, col_at), (P_SIZE, P_SIZE))
            obj_den = lax.dynamic_update_slice(obj_den, current_den + weight * probe_power, (row_at, col_at))
            pr_num = pr_num + jnp.conj(patch) * gap
            pr_den = pr_den + weight * (patch.real * patch.real + patch.imag * patch.imag)
            return ((obj_num, obj_den, pr_num, pr_den), None)
        start = (jnp.zeros(field.shape, field.dtype), jnp.zeros(field.shape, ftype), probe_num, probe_den)
        (obj_num, obj_den, probe_num, probe_den), _ = lax.scan(deposit, start, (spots, weights, measured))
        numerators.append(obj_num)
        denominators.append(obj_den)
        fields.append(field)
    peak_obj = jnp.max(jnp.stack([jnp.max(den) for den in denominators]))
    peak_probe = jnp.max(probe_den)
    updated = []
    for angle_index in range(ANGLES):
        value = fields[angle_index] + numerators[angle_index] / (denominators[angle_index] + 0.1 * peak_obj)
        updated.append(jnp.stack([value.real, value.imag]))
    new_object = jnp.stack(updated)
    probe_new = probe_wave + probe_num / (probe_den + 0.1 * peak_probe)
    new_probe = jnp.stack([probe_new.real, probe_new.imag])
    return (new_object, new_probe)
```

```python
import functools
import math

import jax
import jax.numpy as jnp
import numpy as np
from jax import lax
from jax.experimental import pallas as pl
from jax.experimental.pallas import tpu as pltpu
from jax.sharding import PartitionSpec as P

MESH = pl.DeviceIdType.MESH
LANES = 128
VMEM_LIMIT = 56 * 1024 * 1024
AROUND = tuple((dy, dx) for dy in (-1, 0, 1) for dx in (-1, 0, 1))
BESIDE = tuple(d for d in AROUND if d != (0, 0))
DIAGONALS = tuple(d for d in BESIDE if d[0] and d[1])


def slot_of(dy, dx):
    return (dy + 1) * 3 + dx + 1


def present(dy, dx, shape):
    row = lax.axis_index("ty") + dy
    col = lax.axis_index("tx") + dx
    return (row >= 0) & (row < shape["ty"]) & (col >= 0) & (col < shape["tx"])


def beside_counts(shape):
    found = []
    for axis in ("ty", "tx"):
        at = lax.axis_index(axis)
        found.append(jnp.where(at > 0, 1, 0) + jnp.where(at < shape[axis] - 1, 1, 0))
    return found


def neighbour(dy, dx):
    return {"ty": lax.axis_index("ty") + dy, "tx": lax.axis_index("tx") + dx}


def edge_part(step, size, half):
    return {-1: (half, half), 0: (half, size), 1: (size, half)}[step]


def wide_part(step, size, half):
    return {-1: (0, half), 0: (half, size), 1: (half + size, half)}[step]


def region(ref, rows, blocks):
    return ref.at[:, pl.ds(*blocks), pl.ds(*rows), :]


def split(value):
    high = value.astype(jnp.bfloat16)
    low = (value - high.astype(jnp.float32)).astype(jnp.bfloat16)
    return high, low


def mm(a, b):
    return lax.dot_general(a, b, (((1,), (0,)), ((), ())), preferred_element_type=jnp.float32)


def cat(parts, axis):
    return jnp.concatenate(parts, axis=axis)


def step_kernel(
        shape, pos, live, tile_in, probe_in, counts_in, tables_in,
        out, out_probe,
        wide, tot, den, dbuf, metas, smetas, probe, counts, amp, tables, mats,
        sums, rim_v, rim_h, rim_c, r1, s1, r2, s2, r3, s3, g4, pk_own, pk_a, pk_b, pk_c,
        hsend, hrecv, nsend, nrecv, fsend, frecv, send1, recv1, send2, recv2, send3, recv3, send4, recv4,
        ksend, krecv, lsend, lrecv, msend, mrecv, local, local_tile):
    f32 = jnp.float32
    size = probe.shape[1]
    half = size // 2
    slots = counts.shape[0]
    rows, cols = tile_in.shape[1], tile_in.shape[2]
    inner = cols // LANES
    margin = half // LANES
    blocks = inner + 2 * margin
    pieces = size // LANES
    span = pieces + 1
    n_ty, n_tx, n_an = shape["ty"], shape["tx"], shape["angle"]
    ty, tx, an = lax.axis_index("ty"), lax.axis_index("tx"), lax.axis_index("angle")
    core, z = ty % 2, ty // 2
    n_z = n_ty // 2
    group = n_an * n_tx
    gid = an * n_tx + tx
    each = size // n_ty
    part = sums.shape[3] // n_an

    load_tile = [
        pltpu.make_async_copy(
            tile_in.at[:, :, pl.ds(j * LANES, LANES)],
            wide.at[:, margin + j, pl.ds(half, rows), :], local_tile.at[j])
        for j in range(inner)]
    load_probe = pltpu.make_async_copy(probe_in, probe, local.at[0])
    load_counts = [
        pltpu.make_async_copy(counts_in.at[:, :, pl.ds(b * LANES, LANES)], counts.at[:, b], local.at[4 + b])
        for b in range(pieces)]
    load_tables = pltpu.make_async_copy(tables_in, tables, local.at[2])
    for copy in load_tile + load_counts + [load_probe, load_tables]:
        copy.start()

    lane8 = lax.broadcasted_iota(jnp.int32, (8, LANES), 1)
    line = jnp.zeros((8, LANES), jnp.int32)
    for s in range(slots):
        line = jnp.where(lane8 == s, pos[0, s], line)
        line = jnp.where(lane8 == slots + s, pos[1, s], line)
    line = jnp.where(lane8 == 2 * slots, live[0], line)
    for k in range(9):
        metas[k] = line if k == 4 else jnp.zeros((8, LANES), jnp.int32)

    barrier = pltpu.get_barrier_semaphore()

    def signal(where):
        pl.semaphore_signal(barrier, inc=1, device_id=where, device_id_type=MESH)

    def member(d):
        g = (gid + d) % group
        return g, {"angle": g // n_tx, "tx": g % n_tx}

    for d in range(1, n_ty):
        signal({"ty": (ty + d) % n_ty})
    for d in range(1, group):
        signal(member(d)[1])
    for dy, dx in DIAGONALS:
        @pl.when(present(dy, dx, shape))
        def _():
            signal(neighbour(dy, dx))
    for copy in load_tile:
        copy.wait()
    n_row, n_col = beside_counts(shape)
    pl.semaphore_wait(barrier, n_ty - 1 + group - 1 + n_row * n_col)

    def rdma(src, dst, s_sem, r_sem, where):
        return pltpu.make_async_remote_copy(
            src_ref=src, dst_ref=dst, send_sem=s_sem, recv_sem=r_sem,
            device_id=where, device_id_type=MESH)

    def halo(dy, dx):
        k = slot_of(dy, dx)
        src = region(wide, edge_part(dy, rows, half), edge_part(dx, inner, margin))
        dst = region(wide, wide_part(-dy, rows, half), wide_part(-dx, inner, margin))
        return rdma(src, dst, hsend.at[k], hrecv.at[k], neighbour(dy, dx))

    def note(dy, dx):
        k = slot_of(dy, dx)
        return rdma(metas.at[4], metas.at[slot_of(-dy, -dx)], nsend.at[k], nrecv.at[k], neighbour(dy, dx))

    order = sorted(BESIDE, key=lambda d: abs(d[1]))
    for dy, dx in order:
        @pl.when(present(dy, dx, shape))
        def _():
            note(dy, dx).start()
    for dy, dx in order:
        @pl.when(present(dy, dx, shape))
        def _():
            halo(dy, dx).start()

    def landing(dy, dx):
        if dx == 0:
            return rim_v.at[(dy + 1) // 2]
        if dy == 0:
            return rim_h.at[(dx + 1) // 2]
        return rim_c.at[(dy + 1) + (dx + 1) // 2]

    for dy, dx in BESIDE:
        @pl.when(jnp.logical_not(present(dy, dx, shape)))
        def _():
            place = landing(-dy, -dx)
            place[...] = jnp.zeros(place.shape, f32)

    def clear(n, carry):
        s, ch = n // 2, n % 2
        tall = dbuf.shape[3]
        for b in (0, span + 1):
            dbuf[s, ch, b] = jnp.zeros((tall, LANES), f32)
        for b in range(1, span + 1):
            dbuf[s, ch, b, 0:size, :] = jnp.zeros((size, LANES), f32)
            dbuf[s, ch, b, 2 * size:, :] = jnp.zeros((tall - 2 * size, LANES), f32)
        return carry

    lax.fori_loop(0, 2 * slots, clear, 0)
    den[...] = jnp.zeros_like(den)
    sums[...] = jnp.zeros_like(sums)

    load_probe.wait()
    for dy, dx in order:
        @pl.when(present(dy, dx, shape))
        def _():
            note(dy, dx).wait_send()
            note(-dy, -dx).wait_recv()
    to_scalar = pltpu.make_async_copy(metas, smetas, local.at[3])
    to_scalar.start()
    to_scalar.wait()

    lane = lax.broadcasted_iota(jnp.int32, (size, LANES), 1)

    def spread(piece, shift):
        moved = [pltpu.roll(piece[:, b * LANES:(b + 1) * LANES], shift, axis=1) for b in range(pieces)]
        low = lane < shift
        found = [jnp.where(low, 0.0, moved[0])]
        for b in range(1, pieces):
            found.append(jnp.where(low, moved[b - 1], moved[b]))
        found.append(jnp.where(low, moved[-1], 0.0))
        return found

    def spot(k, s):
        return smetas[k, 0, s] - ty * rows + half, smetas[k, 0, slots + s] - tx * cols + half

    far = 64 * LANES

    def place(k, s):
        dy, dx = k // 3 - 1, k % 3 - 1
        row, at = spot(k, s)
        row = jnp.clip(row, dy * rows, dy * rows + rows - 1)
        at = jnp.clip(at, dx * cols, dx * cols + cols - 1)
        first = (at + far * LANES) // LANES - far
        return row, first, (at + far * LANES) % LANES

    power = probe[0] * probe[0] + probe[1] * probe[1]
    base = size

    def gathered(ch, j, start, count, spots):
        total = None
        for s, (row, first, _) in enumerate(spots):
            b = jnp.clip(j - first + 1, 0, span + 1)
            value = dbuf[s, ch, b, pl.ds(start - row + base, count), :]
            total = value if total is None else total + value
        return total

    chunk = half
    for k, (dy, dx) in enumerate(AROUND):
        there = present(dy, dx, shape)
        spots = [place(k, s) for s in range(slots)]

        def fill(s, carry):
            row, first, shift = place(k, s)
            used = there & (s < smetas[k, 0, 2 * slots])
            for b, value in enumerate(spread(jnp.where(used, power, 0.0), shift)):
                dbuf[s, 0, 1 + b, size:2 * size, :] = value
            return carry

        lax.fori_loop(0, slots, fill, 0)
        tall = range(0, rows, chunk) if dy == 0 else (range(0, half, chunk) if dy < 0 else range(rows - half, rows, chunk))
        if dx == 0:
            def column(j, carry):
                for r in tall:
                    den[j, r:r + chunk, :] += gathered(0, j + margin, half + r, chunk, spots)
                return carry

            lax.fori_loop(0, inner, column, 0)
        else:
            for j in range(margin) if dx < 0 else range(inner - margin, inner):
                for r in tall:
                    den[j, r:r + chunk, :] += gathered(0, j + margin, half + r, chunk, spots)

    def top(value):
        return jnp.max(jnp.max(value, axis=0, keepdims=True), axis=1, keepdims=True)

    pk_own[...] = jnp.broadcast_to(top(jnp.max(den[...], axis=0)), pk_own.shape)
    pk_a[pl.ds(gid, 1)] = pk_own[...][None]
    for d in range(1, group):
        g, where = member(d)
        rdma(pk_own, pk_a.at[gid], ksend.at[d], krecv.at[gid], where).start()

    load_tables.wait()
    for n in range(2):
        ce, se, co, so, cot, sot = [tables[6 * n + i] for i in range(6)]
        for m, (c, up, down) in enumerate(((ce, se, -se), (co, so, -so), (ce, -se, se), (cot, -sot, sot))):
            mats[n, m, 0:half, 0:half] = c
            mats[n, m, 0:half, half:] = up
            mats[n, m, half:, 0:half] = down
            mats[n, m, half:, half:] = c

    for copy in load_counts:
        copy.wait()
    from_lane = lax.broadcasted_iota(jnp.int32, (size, size), 0)
    to_lane = lax.broadcasted_iota(jnp.int32, (size, size), 1)
    wanted = jnp.where(to_lane < half, 2 * to_lane, 2 * (to_lane - half) + 1)
    shuffle = jnp.where(from_lane == wanted, 1.0, 0.0).astype(jnp.bfloat16)
    shuffle2 = cat([shuffle, shuffle], 0)

    def amplitude(s, carry):
        seen = cat([
            cat([counts[s, b, pl.ds(n, half, stride=2), :] for b in range(pieces)], 1) for n in range(2)], 0).astype(f32)
        amp[s] = 0.05 * jnp.sqrt(mm(cat(list(split(seen)), 1), shuffle2))
        return carry

    lax.fori_loop(0, slots, amplitude, 0)

    for d in range(1, group):
        g, where = member(d)
        rdma(pk_own, pk_a.at[g], ksend.at[d], krecv.at[g], where).wait()
    peak = pk_a[0]
    for g in range(1, group):
        peak = jnp.maximum(peak, pk_a[g])
    pk_b[pl.ds(ty, 1)] = peak[None]
    for d in range(1, n_ty):
        rdma(pk_b.at[ty], pk_b.at[ty], lsend.at[d], lrecv.at[ty], {"ty": (ty + d) % n_ty}).start()
    for d in range(1, n_ty):
        o = (ty + d) % n_ty
        rdma(pk_b.at[ty], pk_b.at[o], lsend.at[d], lrecv.at[o], {"ty": o}).wait()
    peak = pk_b[0]
    for t in range(1, n_ty):
        peak = jnp.maximum(peak, pk_b[t])
    den[...] = 1.0 / (den[...] + 0.1 * peak[0:1, 0:1])

    for dy, dx in order:
        @pl.when(present(dy, dx, shape))
        def _():
            halo(dy, dx).wait_send()
            halo(-dy, -dx).wait_recv()

    def matrix(m, axis):
        return cat([mats[0, m], mats[0, m], mats[1, m]], axis)

    def from_left(m, re, im):
        high, low = split(cat([re, im], 0))
        found = mm(matrix(m, 1), cat([high, low, high], 0))
        return found[:half], found[half:]

    def from_right(m, re, im):
        high, low = split(cat([re, im], 1))
        found = mm(cat([high, low, high], 1), matrix(m, 0))
        return found[:, :half], found[:, half:]

    def one_slot(s, carry):
        row, first, shift = place(4, s)
        used = s < smetas[4, 0, 2 * slots]
        back = (LANES - shift) % LANES
        keep = lane < LANES - shift

        def patch(ch):
            moved = [
                pltpu.roll(wide[ch, first + b, pl.ds(row, size), :], back, axis=1)
                for b in range(span)]
            return cat([jnp.where(keep, moved[b], moved[b + 1]) for b in range(pieces)], 1)

        x_re, x_im = patch(0), patch(1)
        q_re, q_im = probe[0], probe[1]
        p_re = q_re * x_re - q_im * x_im
        p_im = q_re * x_im + q_im * x_re
        a = from_left(0, p_re[:half] + p_re[half:], p_im[:half] + p_im[half:])
        b = from_left(1, p_re[:half] - p_re[half:], p_im[:half] - p_im[half:])
        y_re, y_im = cat([a[0], b[0]], 0), cat([a[1], b[1]], 0)
        a = from_right(2, y_re[:, :half] + y_re[:, half:], y_im[:, :half] + y_im[:, half:])
        b = from_right(3, y_re[:, :half] - y_re[:, half:], y_im[:, :half] - y_im[:, half:])
        f_re, f_im = cat([a[0], b[0]], 1), cat([a[1], b[1]], 1)
        factor = amp[s] * lax.rsqrt(jnp.maximum(f_re * f_re + f_im * f_im, 0.0625))
        g_re, g_im = f_re * factor, f_im * factor
        a = from_left(2, g_re[:half], g_im[:half])
        b = from_left(3, g_re[half:], g_im[half:])
        y_re, y_im = cat([a[0] + b[0], a[0] - b[0]], 0), cat([a[1] + b[1], a[1] - b[1]], 0)
        a = from_right(0, y_re[:, :half], y_im[:, :half])
        b = from_right(1, y_re[:, half:], y_im[:, half:])
        b_re, b_im = cat([a[0] + b[0], a[0] - b[0]], 1), cat([a[1] + b[1], a[1] - b[1]], 1)
        d_re, d_im = jnp.where(used, b_re - p_re, 0.0), jnp.where(used, b_im - p_im, 0.0)
        for ch, value in enumerate((q_re * d_re + q_im * d_im, q_re * d_im - q_im * d_re)):
            for i, moved in enumerate(spread(value, shift)):
                dbuf[s, ch, 1 + i, size:2 * size, :] = moved
        weighed = (
            x_re * d_re + x_im * d_im,
            x_re * d_im - x_im * d_re,
            jnp.where(used, x_re * x_re + x_im * x_im, 0.0))
        for t in range(n_ty):
            for ch in range(3):
                sums[t % 2, t // 2, ch * each:(ch + 1) * each, :] += weighed[ch][t * each:(t + 1) * each, :]
        return carry

    lax.fori_loop(0, slots, one_slot, 0)

    spots = [place(4, s) for s in range(slots)]
    pair = {"ty": ty + 1 - 2 * core}
    c1 = rdma(sums.at[1 - core], r1, send1.at[0], recv1.at[0], pair)
    c1.start()

    def total_at(start, count, lowest, number):
        def column(n, carry):
            j = lowest + n // 2
            ch = n % 2
            for r in range(start, start + count, chunk):
                tot[ch, j, r:r + chunk, :] = gathered(ch, j, r, chunk, spots)
            return carry

        lax.fori_loop(0, 2 * number, column, 0)

    total_at(0, half, 0, blocks)
    total_at(half + rows, half, 0, blocks)
    total_at(half, rows, 0, margin)
    total_at(half, rows, margin + inner, margin)

    early = half * 5 // 8 // 8 * 8

    def fold(dy, dx, piece=0):
        k = slot_of(dy, dx) + 9 * piece
        part_rows, part_cols = wide_part(dy, rows, half), wide_part(dx, inner, margin)
        place = landing(dy, dx)
        if dx == 0:
            begin, stop = (0, early) if piece == 0 else (early, half)
            part_rows = (part_rows[0] + begin, stop - begin)
            place = place.at[:, :, pl.ds(begin, stop - begin), :]
        return rdma(region(tot, part_rows, part_cols), place, fsend.at[k], frecv.at[k], neighbour(dy, dx))

    def start_folds(which):
        for dy, dx, piece in which:
            @pl.when(present(dy, dx, shape))
            def _():
                fold(dy, dx, piece).start()

    start_folds([(-1, 0, 0), (1, 0, 0), (0, -1, 0), (0, 1, 0)])

    c1.wait()
    s1[...] = sums[core] + r1[...]

    def lanes(ref, a):
        return ref.at[:, :, pl.ds(pl.multiple_of(a * part, part), part)]

    for d in range(1, n_an):
        a = (an + d) % n_an
        rdma(lanes(s1, a), r2.at[an], send2.at[d], recv2.at[an], {"angle": a}).start()

    def centre_column(j, carry):
        for ch in range(2):
            for r in range(half, half + rows, chunk):
                tot[ch, j + margin, r:r + chunk, :] = gathered(ch, j + margin, r, chunk, spots)
        return carry

    lax.fori_loop(0, inner, centre_column, 0)

    for d in range(1, n_an):
        a = (an + d) % n_an
        rdma(lanes(s1, a), r2.at[a], send2.at[d], recv2.at[a], {"angle": a}).wait()
    mine = s1[:, :, pl.ds(pl.multiple_of(an * part, part), part)]
    for d in range(1, n_an):
        mine = mine + r2[(an + d) % n_an]
    s2[...] = mine

    for d in range(1, n_z):
        o = (z + d) % n_z
        rdma(s2.at[o], r3.at[z], send3.at[d], recv3.at[z], {"ty": o * 2 + core}).start()
    start_folds([(-1, 0, 1), (1, 0, 1)] + [(dy, dx, 0) for dy, dx in DIAGONALS])
    for d in range(1, n_z):
        o = (z + d) % n_z
        rdma(s2.at[o], r3.at[o], send3.at[d], recv3.at[o], {"ty": o * 2 + core}).wait()
    total = s2[z]
    for d in range(1, n_z):
        total = total + r3[(z + d) % n_z]
    s3[...] = total
    g4[pl.ds(gid, 1)] = total[None]

    for d in range(1, group):
        g, where = member(d)
        rdma(s3, g4.at[gid], send4.at[d], recv4.at[gid], where).start()
    for d in range(1, group):
        g, where = member(d)
        rdma(s3, g4.at[g], send4.at[d], recv4.at[g], where).wait()
    found = []
    for a in range(n_an):
        piece = g4[a * n_tx]
        for t in range(1, n_tx):
            piece = piece + g4[a * n_tx + t]
        found.append(piece)
    full = cat(found, 1)
    p_re, p_im, p_den = full[:each], full[each:2 * each], full[2 * each:]

    pk_c[pl.ds(ty, 1)] = jnp.broadcast_to(top(p_den), pk_own.shape)[None]
    for d in range(1, n_ty):
        rdma(pk_c.at[ty], pk_c.at[ty], msend.at[d], mrecv.at[ty], {"ty": (ty + d) % n_ty}).start()

    for dy, dx in BESIDE:
        @pl.when(present(dy, dx, shape))
        def _():
            for piece in (0, 1) if dx == 0 else (0,):
                fold(dy, dx, piece).wait_send()
                fold(-dy, -dx, piece).wait_recv()

    def final(ch, j, extra):
        for r in range(0, rows, chunk):
            value = tot[ch, j + margin, half + r:half + r + chunk, :]
            for r_from, c_from, found in extra:
                if r_from == 0 or (r_from < 0 and r < half) or (r_from > 0 and r >= rows - half):
                    at = r if r_from <= 0 else r - (rows - half)
                    value = value + found(ch, j, at)
            own = wide[ch, j + margin, half + r:half + r + chunk, :]
            yield r, own + value * den[j, r:r + chunk, :]

    def from_rim(dy, dx):
        place = landing(-dy, -dx)
        lowest = inner - margin if dx > 0 else 0
        return dy, dx, lambda ch, j, at: place[ch, j - lowest, at:at + chunk, :]

    for j in range(inner):
        here = [(-1, 0), (1, 0)]
        if j < margin:
            here += [(dy, -1) for dy in (-1, 0, 1)]
        if j >= inner - margin:
            here += [(dy, 1) for dy in (-1, 0, 1)]
        for ch in range(2):
            for r, value in final(ch, j, [from_rim(dy, dx) for dy, dx in here]):
                out[ch, r:r + chunk, j * LANES:(j + 1) * LANES] = value

    for d in range(1, n_ty):
        o = (ty + d) % n_ty
        rdma(pk_c.at[ty], pk_c.at[o], msend.at[d], mrecv.at[o], {"ty": o}).wait()
    peak = pk_c[0]
    for t in range(1, n_ty):
        peak = jnp.maximum(peak, pk_c[t])
    scale = 1.0 / (p_den + 0.1 * peak[0:1, 0:1])
    own_rows = pl.ds(pl.multiple_of(ty * each, each), each)
    out_probe[0] = probe[0, own_rows, :] + p_re * scale
    out_probe[1] = probe[1, own_rows, :] + p_im * scale


def table_values(length):
    half = length // 2
    j, m = np.arange(half), np.arange(half)
    even = 2.0 * math.pi / length * (np.outer(2 * m, j) % length)
    odd = 2.0 * math.pi / length * (np.outer(2 * m + 1, j) % length)
    values = []
    for phase in (even, odd, odd.T):
        values += [np.cos(phase) / math.sqrt(length), np.sin(phase) / math.sqrt(length)]
    high = [value.astype(jnp.bfloat16) for value in values]
    low = [(value - h.astype(np.float64)).astype(jnp.bfloat16) for value, h in zip(values, high)]
    return np.stack(high + low)


def body(shape, object_slices, probe_field, positions, live_slots, photon_counts):
    f32 = jnp.float32
    dma = pltpu.SemaphoreType.DMA
    size = probe_field.shape[1]
    half = size // 2
    tile = object_slices[0]
    _, rows, cols = tile.shape
    spots = positions[0, 0, 0].T
    slots = spots.shape[1]
    inner, margin = cols // LANES, half // LANES
    blocks = inner + 2 * margin
    span = size // LANES + 1
    n_ty, n_tx, n_an = shape["ty"], shape["tx"], shape["angle"]
    n_z, each, group = n_ty // 2, size // n_ty, n_an * n_tx
    part = size // n_an
    vmem = pl.BlockSpec(memory_space=pltpu.VMEM)
    smem = pl.BlockSpec(memory_space=pltpu.SMEM)
    hbm = pl.BlockSpec(memory_space=pltpu.HBM)

    return pl.pallas_call(
        functools.partial(step_kernel, shape),
        out_shape=(
            jax.ShapeDtypeStruct((2, rows, cols), f32),
            jax.ShapeDtypeStruct((2, each, size), f32),
        ),
        in_specs=[smem, smem, hbm, hbm, hbm, hbm],
        out_specs=(vmem, vmem),
        scratch_shapes=[
            pltpu.VMEM((2, blocks, rows + size, LANES), f32),
            pltpu.VMEM((2, blocks, rows + size, LANES), f32),
            pltpu.VMEM((inner, rows, LANES), f32),
            pltpu.VMEM((slots, 2, span + 2, rows + 2 * size, LANES), f32),
            pltpu.VMEM((9, 8, LANES), jnp.int32),
            pltpu.SMEM((9, 8, LANES), jnp.int32),
            pltpu.VMEM((2, size, size), f32),
            pltpu.VMEM((slots, size // LANES, size, LANES), jnp.int32),
            pltpu.VMEM((slots, size, size), f32),
            pltpu.VMEM((12, half, half), jnp.bfloat16),
            pltpu.VMEM((2, 4, size, size), jnp.bfloat16),
            pltpu.VMEM((2, n_z, 3 * each, size), f32),
            pltpu.VMEM((2, 2, inner, half, LANES), f32),
            pltpu.VMEM((2, 2, margin, rows, LANES), f32),
            pltpu.VMEM((4, 2, margin, half, LANES), f32),
            pltpu.VMEM((n_z, 3 * each, size), f32),
            pltpu.VMEM((n_z, 3 * each, size), f32),
            pltpu.VMEM((n_an, n_z, 3 * each, part), f32),
            pltpu.VMEM((n_z, 3 * each, part), f32),
            pltpu.VMEM((n_z, 3 * each, part), f32),
            pltpu.VMEM((3 * each, part), f32),
            pltpu.VMEM((group, 3 * each, part), f32),
            pltpu.VMEM((8, LANES), f32),
            pltpu.VMEM((group, 8, LANES), f32),
            pltpu.VMEM((n_ty, 8, LANES), f32),
            pltpu.VMEM((n_ty, 8, LANES), f32),
            dma((9,)), dma((9,)), dma((9,)), dma((9,)),
            dma((18,)), dma((18,)), dma((1,)), dma((1,)), dma((n_an,)), dma((n_an,)),
            dma((n_z,)), dma((n_z,)), dma((group,)), dma((group,)),
            dma((group,)), dma((group,)), dma((n_ty,)), dma((n_ty,)), dma((n_ty,)), dma((n_ty,)),
            dma((4 + size // LANES,)), dma((inner,)),
        ],
        compiler_params=pltpu.CompilerParams(
            collective_id=0, has_side_effects=True, vmem_limit_bytes=VMEM_LIMIT),
    )(spots, live_slots[0, 0], tile, probe_field, photon_counts[0, 0, 0], jnp.asarray(table_values(size)))


def solution(mesh):
    shape = dict(mesh.shape)

    def step(*args):
        new_tile, new_probe = body(shape, *args)
        return new_tile[None], new_probe

    return jax.shard_map(
        step,
        mesh=mesh,
        in_specs=(
            P("angle", None, "ty", "tx"),
            P(),
            P("angle", "ty", "tx", None, None),
            P("angle", "ty", "tx"),
            P("angle", "ty", "tx", None, None, None),
        ),
        out_specs=(P("angle", None, "ty", "tx"), P(None, "ty", None)),
        check_vma=False,
    )
```

```python
import functools
import math

import jax
import jax.numpy as jnp
import numpy as np
from jax import lax
from jax.experimental import pallas as pl
from jax.experimental.pallas import tpu as pltpu
from jax.sharding import PartitionSpec as P

MESH = pl.DeviceIdType.MESH
LANES = 128
VMEM_LIMIT = 44 * 1024 * 1024
FINISH_LIMIT = 4 * 1024 * 1024
AROUND = tuple((dy, dx) for dy in (-1, 0, 1) for dx in (-1, 0, 1))
BESIDE = tuple(d for d in AROUND if d != (0, 0))
DIAGONALS = tuple(d for d in BESIDE if d[0] and d[1])


def slot_of(dy, dx):
    return (dy + 1) * 3 + dx + 1


def present(dy, dx, shape):
    row = lax.axis_index("ty") + dy
    col = lax.axis_index("tx") + dx
    return (row >= 0) & (row < shape["ty"]) & (col >= 0) & (col < shape["tx"])


def beside_counts(shape):
    found = []
    for axis in ("ty", "tx"):
        at = lax.axis_index(axis)
        found.append(jnp.where(at > 0, 1, 0) + jnp.where(at < shape[axis] - 1, 1, 0))
    return found


def neighbour(dy, dx):
    return {"ty": lax.axis_index("ty") + dy, "tx": lax.axis_index("tx") + dx}


def edge_part(step, size, half):
    return {-1: (half, half), 0: (half, size), 1: (size, half)}[step]


def wide_part(step, size, half):
    return {-1: (0, half), 0: (half, size), 1: (half + size, half)}[step]


def region(ref, rows, blocks):
    return ref.at[:, pl.ds(*blocks), pl.ds(*rows), :]


def split(value):
    high = value.astype(jnp.bfloat16)
    low = (value - high.astype(jnp.float32)).astype(jnp.bfloat16)
    return high, low


def mm(a, b):
    return lax.dot_general(a, b, (((1,), (0,)), ((), ())), preferred_element_type=jnp.float32)


def cat(parts, axis):
    return jnp.concatenate(parts, axis=axis)


def step_kernel(
        shape, live, pos_in, tile_in, probe_in, counts_in, tables_in,
        out, out_probe,
        pos, wide, tot, den, dbuf, metas, smetas, probe, counts, amp, tables, mats,
        xbuf, rim_v, rim_h, pk_own, pk_a, pk_b, pk_c,
        hsend, hrecv, nsend, nrecv, fsend, frecv, ksend, krecv, lsend, lrecv, msend, mrecv, local, local_tile,
        *chain_refs):
    f32 = jnp.float32
    size = probe.shape[1]
    half = size // 2
    slots = counts.shape[0]
    rows, cols = tile_in.shape[1], tile_in.shape[2]
    inner = cols // LANES
    margin = half // LANES
    blocks = inner + 2 * margin
    pieces = size // LANES
    span = pieces + 1
    n_ty, n_tx, n_an = shape["ty"], shape["tx"], shape["angle"]
    ty, tx, an = lax.axis_index("ty"), lax.axis_index("tx"), lax.axis_index("angle")
    core, z = ty % 2, ty // 2
    n_z = n_ty // 2
    group = n_an * n_tx
    gid = an * n_tx + tx
    each = size // n_ty
    part = size // n_an
    den_refs, num_refs = chain_refs[:len(chain_refs) // 2], chain_refs[len(chain_refs) // 2:]
    sums_d, sums_n = den_refs[0], num_refs[0]

    load_pos = pltpu.make_async_copy(pos_in, pos, local.at[3])
    load_pos.start()
    load_tile = [
        pltpu.make_async_copy(
            tile_in.at[:, :, pl.ds(j * LANES, LANES)],
            wide.at[:, margin + j, pl.ds(half, rows), :], local_tile.at[j])
        for j in range(inner)]
    load_probe = pltpu.make_async_copy(probe_in, probe, local.at[0])
    load_counts = [
        pltpu.make_async_copy(counts_in.at[:, :, pl.ds(b * LANES, LANES)], counts.at[:, b], local.at[4 + b])
        for b in range(pieces)]
    load_tables = pltpu.make_async_copy(tables_in, tables, local.at[2])
    for copy in load_tile + load_counts + [load_probe, load_tables]:
        copy.start()

    load_pos.wait()
    lane8 = lax.broadcasted_iota(jnp.int32, (8, LANES), 1)
    line = jnp.zeros((8, LANES), jnp.int32)
    for s in range(slots):
        line = jnp.where(lane8 == s, pos[0, s], line)
        line = jnp.where(lane8 == slots + s, pos[1, s], line)
    line = jnp.where(lane8 == 2 * slots, live[0, 0], line)
    for k in range(9):
        metas[k] = line if k == 4 else jnp.zeros((8, LANES), jnp.int32)

    barrier = pltpu.get_barrier_semaphore()

    def signal(where):
        pl.semaphore_signal(barrier, inc=1, device_id=where, device_id_type=MESH)

    def member(d):
        g = (gid + d) % group
        return g, {"angle": g // n_tx, "tx": g % n_tx}

    for d in range(1, n_ty):
        signal({"ty": (ty + d) % n_ty})
    for d in range(1, group):
        signal(member(d)[1])
    for dy, dx in DIAGONALS:
        @pl.when(present(dy, dx, shape))
        def _():
            signal(neighbour(dy, dx))
    def landing(dy, dx):
        return rim_v.at[(dy + 1) // 2] if dx == 0 else rim_h.at[(dx + 1) // 2]

    for dy, dx in ((-1, 0), (1, 0), (0, -1), (0, 1)):
        @pl.when(jnp.logical_not(present(dy, dx, shape)))
        def _():
            place = landing(-dy, -dx)
            place[...] = jnp.zeros(place.shape, f32)

    for dy, dx in BESIDE:
        @pl.when(jnp.logical_not(present(dy, dx, shape)))
        def _():
            place = landing(-dy, -dx)
            place[...] = jnp.zeros(place.shape, f32)

    def clear(n, carry):
        s, ch = n // 2, n % 2
        tall = dbuf.shape[3]
        for b in (0, span + 1):
            dbuf[s, ch, b] = jnp.zeros((tall, LANES), f32)
        for b in range(1, span + 1):
            dbuf[s, ch, b, 0:size, :] = jnp.zeros((size, LANES), f32)
            dbuf[s, ch, b, 2 * size:, :] = jnp.zeros((tall - 2 * size, LANES), f32)
        return carry

    lax.fori_loop(0, 2 * slots, clear, 0)
    den[...] = jnp.zeros_like(den)
    sums_d[...] = jnp.zeros_like(sums_d)
    sums_n[...] = jnp.zeros_like(sums_n)

    load_tables.wait()
    for n in range(2):
        ce, se, co, so, cot, sot = [tables[6 * n + i] for i in range(6)]
        for m, (c, up, down) in enumerate(((ce, se, -se), (co, so, -so), (ce, -se, se), (cot, -sot, sot))):
            mats[n, m, 0:half, 0:half] = c
            mats[n, m, 0:half, half:] = up
            mats[n, m, half:, 0:half] = down
            mats[n, m, half:, half:] = c

    for copy in load_tile:
        copy.wait()
    n_row, n_col = beside_counts(shape)
    pl.semaphore_wait(barrier, n_ty - 1 + group - 1 + n_row * n_col)

    def rdma(src, dst, s_sem, r_sem, where):
        return pltpu.make_async_remote_copy(
            src_ref=src, dst_ref=dst, send_sem=s_sem, recv_sem=r_sem,
            device_id=where, device_id_type=MESH)

    strips = ((margin, margin), (inner, margin), (2 * margin, inner - 2 * margin))
    SIDES = ((-1, 0), (1, 0), (0, -1), (0, 1))

    def halo_v(dy, i):
        src = region(wide, edge_part(dy, rows, half), strips[i])
        dst = region(wide, wide_part(-dy, rows, half), strips[i])
        k = (dy + 1) // 2 * len(strips) + i
        return rdma(src, dst, hsend.at[k], hrecv.at[k], neighbour(dy, 0))

    def halo_h(dx, dy):
        part_rows = wide_part(dy, rows, half)
        src = region(wide, part_rows, edge_part(dx, inner, margin))
        dst = region(wide, part_rows, wide_part(-dx, inner, margin))
        k = 2 * len(strips) + (dx + 1) // 2 * 3 + dy + 1
        return rdma(src, dst, hsend.at[k], hrecv.at[k], neighbour(0, dx))

    def note(dy, dx):
        k = slot_of(dy, dx)
        return rdma(metas.at[4], metas.at[slot_of(-dy, -dx)], nsend.at[k], nrecv.at[k], neighbour(dy, dx))

    order = sorted(BESIDE, key=lambda d: abs(d[1]))
    for dy, dx in order:
        @pl.when(present(dy, dx, shape))
        def _():
            note(dy, dx).start()
    for dy, dx in SIDES:
        @pl.when(present(dy, dx, shape))
        def _():
            if dx == 0:
                halo_v(dy, 0).start()
                halo_v(dy, 1).start()
            else:
                halo_h(dx, 0).start()
    for dy in (-1, 1):
        @pl.when(present(dy, 0, shape))
        def _():
            halo_v(dy, 2).start()

    for copy in load_counts:
        copy.wait()
    from_lane = lax.broadcasted_iota(jnp.int32, (size, size), 0)
    to_lane = lax.broadcasted_iota(jnp.int32, (size, size), 1)
    wanted = jnp.where(to_lane < half, 2 * to_lane, 2 * (to_lane - half) + 1)
    shuffle = jnp.where(from_lane == wanted, 1.0, 0.0).astype(jnp.bfloat16)
    shuffle2 = cat([shuffle, shuffle], 0)

    def amplitude(s, carry):
        seen = cat([
            cat([counts[s, b, pl.ds(n, half, stride=2), :] for b in range(pieces)], 1) for n in range(2)], 0).astype(f32)
        amp[s] = 0.05 * jnp.sqrt(mm(cat(list(split(seen)), 1), shuffle2))
        return carry

    lax.fori_loop(0, slots, amplitude, 0)

    load_probe.wait()
    for dy, dx in order:
        @pl.when(present(dy, dx, shape))
        def _():
            note(dy, dx).wait_send()
            note(-dy, -dx).wait_recv()
    for dy in (-1, 1):
        @pl.when(present(dy, 0, shape))
        def _():
            halo_v(-dy, 0).wait_recv()
            halo_v(-dy, 1).wait_recv()
    for dy, dx in DIAGONALS:
        @pl.when(present(dy, dx, shape))
        def _():
            halo_h(dx, dy).start()
    to_scalar = pltpu.make_async_copy(metas, smetas, local.at[3])
    to_scalar.start()
    to_scalar.wait()

    lane = lax.broadcasted_iota(jnp.int32, (size, LANES), 1)

    def spread(piece, shift):
        moved = [pltpu.roll(piece[:, b * LANES:(b + 1) * LANES], shift, axis=1) for b in range(pieces)]
        low = lane[:piece.shape[0]] < shift
        found = [jnp.where(low, 0.0, moved[0])]
        for b in range(1, pieces):
            found.append(jnp.where(low, moved[b - 1], moved[b]))
        found.append(jnp.where(low, moved[-1], 0.0))
        return found

    def spot(k, s):
        return smetas[k, 0, s] - ty * rows + half, smetas[k, 0, slots + s] - tx * cols + half

    far = 64 * LANES

    def place(k, s):
        dy, dx = k // 3 - 1, k % 3 - 1
        row, at = spot(k, s)
        row = jnp.clip(row, dy * rows, dy * rows + rows - 1)
        at = jnp.clip(at, dx * cols, dx * cols + cols - 1)
        first = (at + far * LANES) // LANES - far
        return row, first, (at + far * LANES) % LANES

    power = probe[0] * probe[0] + probe[1] * probe[1]
    base = size

    def gathered(ch, j, start, count, spots):
        total = None
        for s, (row, first, _) in enumerate(spots):
            b = jnp.clip(j - first + 1, 0, span + 1)
            value = dbuf[s, ch, b, pl.ds(start - row + base, count), :]
            total = value if total is None else total + value
        return total

    chunk = half
    for k, (dy, dx) in enumerate(AROUND):
        there = present(dy, dx, shape)
        spots = [place(k, s) for s in range(slots)]

        part_rows = {-1: (half, size), 0: (0, size), 1: (0, half)}[dy]
        for s in range(slots):
            used = there & (s < smetas[k, 0, 2 * slots])
            piece = jnp.where(used, power[part_rows[0]:part_rows[1]], 0.0)
            for b, value in enumerate(spread(piece, spots[s][2])):
                dbuf[s, 0, 1 + b, size + part_rows[0]:size + part_rows[1], :] = value
        tall = range(0, rows, chunk) if dy == 0 else (range(0, half, chunk) if dy < 0 else range(rows - half, rows, chunk))
        if dx == 0:
            def column(j, carry):
                for r in tall:
                    den[j, r:r + chunk, :] += gathered(0, j + margin, half + r, chunk, spots)
                return carry

            lax.fori_loop(0, inner, column, 0)
        else:
            for j in range(margin) if dx < 0 else range(inner - margin, inner):
                for r in tall:
                    den[j, r:r + chunk, :] += gathered(0, j + margin, half + r, chunk, spots)

    def top(value):
        return jnp.max(jnp.max(value, axis=0, keepdims=True), axis=1, keepdims=True)

    pk_own[...] = jnp.broadcast_to(top(jnp.max(den[...], axis=0)), pk_own.shape)
    pk_a[pl.ds(gid, 1)] = pk_own[...][None]
    for d in range(1, group):
        g, where = member(d)
        rdma(pk_own, pk_a.at[gid], ksend.at[d], krecv.at[gid], where).start()

    for dy, dx in SIDES:
        @pl.when(present(dy, dx, shape))
        def _():
            if dx == 0:
                for i in range(len(strips)):
                    halo_v(dy, i).wait_send()
                halo_v(-dy, 2).wait_recv()
            else:
                halo_h(dx, 0).wait_send()
                halo_h(-dx, 0).wait_recv()
    for dy, dx in DIAGONALS:
        @pl.when(present(dy, dx, shape))
        def _():
            halo_h(dx, dy).wait_send()
            halo_h(-dx, dy).wait_recv()

    def matrix(m, axis):
        return cat([mats[0, m], mats[0, m], mats[1, m]], axis)

    def from_left(m, re, im):
        high, low = split(cat([re, im], 0))
        found = mm(matrix(m, 1), cat([high, low, high], 0))
        return found[:half], found[half:]

    def from_right(m, re, im):
        high, low = split(cat([re, im], 1))
        found = mm(cat([high, low, high], 1), matrix(m, 0))
        return found[:, :half], found[:, half:]

    def add_to(total, s, values):
        for t in range(n_ty):
            for ch, value in enumerate(values):
                total[t % 2, t // 2, ch * each:(ch + 1) * each, :] += value[t * each:(t + 1) * each, :]

    def extract(s, carry):
        row, first, shift = place(4, s)
        used = s < smetas[4, 0, 2 * slots]
        back = (LANES - shift) % LANES
        keep = lane < LANES - shift
        found = []
        for ch in range(2):
            moved = [
                pltpu.roll(wide[ch, first + b, pl.ds(row, size), :], back, axis=1)
                for b in range(span)]
            found.append(cat([jnp.where(keep, moved[b], moved[b + 1]) for b in range(pieces)], 1))
            xbuf[s, ch] = found[ch]
        add_to(sums_d, s, (jnp.where(used, found[0] * found[0] + found[1] * found[1], 0.0),))
        return carry

    def one_slot(s, carry):
        shift = place(4, s)[2]
        used = s < smetas[4, 0, 2 * slots]
        x_re, x_im = xbuf[s, 0], xbuf[s, 1]
        q_re, q_im = probe[0], probe[1]
        p_re = q_re * x_re - q_im * x_im
        p_im = q_re * x_im + q_im * x_re
        a = from_left(0, p_re[:half] + p_re[half:], p_im[:half] + p_im[half:])
        b = from_left(1, p_re[:half] - p_re[half:], p_im[:half] - p_im[half:])
        y_re, y_im = cat([a[0], b[0]], 0), cat([a[1], b[1]], 0)
        a = from_right(2, y_re[:, :half] + y_re[:, half:], y_im[:, :half] + y_im[:, half:])
        b = from_right(3, y_re[:, :half] - y_re[:, half:], y_im[:, :half] - y_im[:, half:])
        f_re, f_im = cat([a[0], b[0]], 1), cat([a[1], b[1]], 1)
        factor = amp[s] * lax.rsqrt(jnp.maximum(f_re * f_re + f_im * f_im, 0.0625))
        g_re, g_im = f_re * factor, f_im * factor
        a = from_left(2, g_re[:half], g_im[:half])
        b = from_left(3, g_re[half:], g_im[half:])
        y_re, y_im = cat([a[0] + b[0], a[0] - b[0]], 0), cat([a[1] + b[1], a[1] - b[1]], 0)
        a = from_right(0, y_re[:, :half], y_im[:, :half])
        b = from_right(1, y_re[:, half:], y_im[:, half:])
        b_re, b_im = cat([a[0] + b[0], a[0] - b[0]], 1), cat([a[1] + b[1], a[1] - b[1]], 1)
        d_re, d_im = jnp.where(used, b_re - p_re, 0.0), jnp.where(used, b_im - p_im, 0.0)
        for ch, value in enumerate((q_re * d_re + q_im * d_im, q_re * d_im - q_im * d_re)):
            for i, moved in enumerate(spread(value, shift)):
                dbuf[s, ch, 1 + i, size:2 * size, :] = moved
        add_to(sums_n, s, (x_re * d_re + x_im * d_im, x_re * d_im - x_im * d_re))
        return carry

    def lanes(ref, a):
        return ref.at[:, :, pl.ds(pl.multiple_of(a * part, part), part)]

    class Chain:
        def __init__(self, refs):
            (self.sums, self.r1, self.s1, self.r2, self.s2, self.r3, self.s3, self.g4,
             self.send1, self.recv1, self.send2, self.recv2, self.send3, self.recv3, self.send4, self.recv4) = refs

        def pair(self):
            return rdma(self.sums.at[1 - core], self.r1, self.send1.at[0], self.recv1.at[0], {"ty": ty + 1 - 2 * core})

        def over_angle(self, d, get):
            a = (an + d) % n_an
            return rdma(
                lanes(self.s1, a), self.r2.at[a if get else an], self.send2.at[d],
                self.recv2.at[a if get else an], {"angle": a})

        def over_z(self, d, get):
            o = (z + d) % n_z
            return rdma(
                self.s2.at[o], self.r3.at[o if get else z], self.send3.at[d],
                self.recv3.at[o if get else z], {"ty": o * 2 + core})

        def over_group(self, d, get):
            g, where = member(d)
            at = g if get else gid
            return rdma(self.s3, self.g4.at[at], self.send4.at[d], self.recv4.at[at], where)

        def step1(self):
            self.pair().start()

        def step2(self):
            self.pair().wait()
            self.s1[...] = self.sums[core] + self.r1[...]
            for d in range(1, n_an):
                self.over_angle(d, False).start()

        def step3(self):
            for d in range(1, n_an):
                self.over_angle(d, True).wait()
            total = self.s1[:, :, pl.ds(pl.multiple_of(an * part, part), part)]
            for d in range(1, n_an):
                total = total + self.r2[(an + d) % n_an]
            self.s2[...] = total
            for d in range(1, n_z):
                self.over_z(d, False).start()

        def step4(self):
            for d in range(1, n_z):
                self.over_z(d, True).wait()
            total = self.s2[z]
            for d in range(1, n_z):
                total = total + self.r3[(z + d) % n_z]
            self.s3[...] = total
            self.g4[pl.ds(gid, 1)] = total[None]
            for d in range(1, group):
                self.over_group(d, False).start()

        def result(self):
            for d in range(1, group):
                self.over_group(d, True).wait()
            found = []
            for a in range(n_an):
                piece = self.g4[a * n_tx]
                for t in range(1, n_tx):
                    piece = piece + self.g4[a * n_tx + t]
                found.append(piece)
            return cat(found, 1)

    den_chain, num_chain = Chain(den_refs), Chain(num_refs)
    def some_slots(*which):
        for s in which:
            one_slot(s, 0)

    lax.fori_loop(0, slots, extract, 0)
    den_chain.step1()
    some_slots(0)
    den_chain.step2()
    some_slots(*range(1, slots - 1))
    den_chain.step3()
    some_slots(slots - 1)
    num_chain.step1()

    for d in range(1, group):
        g, where = member(d)
        rdma(pk_own, pk_a.at[g], ksend.at[d], krecv.at[g], where).wait()
    peak = pk_a[0]
    for g in range(1, group):
        peak = jnp.maximum(peak, pk_a[g])
    pk_b[pl.ds(ty, 1)] = peak[None]
    for d in range(1, n_ty):
        rdma(pk_b.at[ty], pk_b.at[ty], lsend.at[d], lrecv.at[ty], {"ty": (ty + d) % n_ty}).start()
    spots = [place(4, s) for s in range(slots)]
    def total_at(start, count, lowest, number):
        def column(n, carry):
            j = lowest + n // 2
            ch = n % 2
            for r in range(start, start + count, chunk):
                tot[ch, j, r:r + chunk, :] = gathered(ch, j, r, chunk, spots)
            return carry

        lax.fori_loop(0, 2 * number, column, 0)

    def fold_h(dx, dy):
        part_rows = wide_part(dy, rows, half)
        k = (dx + 1) // 2 * 3 + dy + 1
        return rdma(
            region(tot, part_rows, wide_part(dx, inner, margin)),
            landing(0, dx).at[:, :, pl.ds(*part_rows), :], fsend.at[k], frecv.at[k], neighbour(0, dx))

    middle = inner - 2 * margin
    first = middle * 2 // 3
    groups = ((2 * margin, first), (2 * margin + first, middle - first), (margin, margin), (inner, margin))

    def fold_v(dy, i):
        start, count = groups[i]
        k = 6 + (dy + 1) // 2 * len(groups) + i
        return rdma(
            region(tot, wide_part(dy, rows, half), groups[i]),
            landing(dy, 0).at[:, pl.ds(start - margin, count)], fsend.at[k], frecv.at[k], neighbour(dy, 0))

    def start_folds_v(which):
        for dy in (-1, 1):
            @pl.when(present(dy, 0, shape))
            def _():
                for i in which:
                    fold_v(dy, i).start()

    def start_folds_h(which):
        for dx in (-1, 1):
            @pl.when(present(0, dx, shape))
            def _():
                for dy in which:
                    fold_h(dx, dy).start()

    total_at(0, half, margin, inner)
    total_at(half + rows, half, margin, inner)
    start_folds_v((0,))
    total_at(0, 2 * half + rows, 0, margin)
    total_at(0, 2 * half + rows, margin + inner, margin)
    start_folds_h((-1,))
    num_chain.step2()
    total_at(half, rows, margin, inner)
    den_chain.step4()
    start_folds_h((1, 0))
    num_chain.step3()
    start_folds_v((1,))
    p_den = den_chain.result()
    pk_c[pl.ds(ty, 1)] = jnp.broadcast_to(top(p_den), pk_own.shape)[None]
    for d in range(1, n_ty):
        rdma(pk_c.at[ty], pk_c.at[ty], msend.at[d], mrecv.at[ty], {"ty": (ty + d) % n_ty}).start()
    for dx in (-1, 1):
        @pl.when(present(0, dx, shape))
        def _():
            for dy in (-1, 1):
                fold_h(-dx, dy).wait_recv()
    for dx in (-1, 1):
        at = edge_part(dx, inner, margin)
        for dy in (-1, 1):
            part_rows = pl.ds(*wide_part(dy, rows, half))
            tot[:, pl.ds(*at), part_rows, :] += landing(0, -dx)[:, :, part_rows, :]
    start_folds_v((2, 3))
    num_chain.step4()
    full = num_chain.result()
    p_re, p_im = full[:each], full[each:]

    for dx in (-1, 1):
        @pl.when(present(0, dx, shape))
        def _():
            for dy in (-1, 1, 0):
                fold_h(dx, dy).wait_send()
            fold_h(-dx, 0).wait_recv()
    for dy in (-1, 1):
        @pl.when(present(dy, 0, shape))
        def _():
            for i in range(len(groups)):
                fold_v(dy, i).wait_send()
                fold_v(-dy, i).wait_recv()

    for d in range(1, n_ty):
        o = (ty + d) % n_ty
        rdma(pk_b.at[ty], pk_b.at[o], lsend.at[d], lrecv.at[o], {"ty": o}).wait()
    peak = pk_b[0]
    for t in range(1, n_ty):
        peak = jnp.maximum(peak, pk_b[t])
    den[...] = 1.0 / (den[...] + 0.1 * peak[0:1, 0:1])

    for j in range(inner):
        for ch in range(2):
            for r in range(0, rows, chunk):
                inside = slice(half + r, half + r + chunk)
                value = tot[ch, j + margin, inside, :]
                if r < half:
                    value = value + landing(1, 0)[ch, j, r:r + chunk, :]
                if r >= rows - half:
                    value = value + landing(-1, 0)[ch, j, r - rows + half:r - rows + half + chunk, :]
                if j < margin:
                    value = value + landing(0, 1)[ch, j, inside, :]
                if j >= inner - margin:
                    value = value + landing(0, -1)[ch, j - inner + margin, inside, :]
                own = wide[ch, j + margin, inside, :]
                out[ch, r:r + chunk, j * LANES:(j + 1) * LANES] = own + value * den[j, r:r + chunk, :]

    for d in range(1, n_ty):
        o = (ty + d) % n_ty
        rdma(pk_c.at[ty], pk_c.at[o], msend.at[d], mrecv.at[o], {"ty": o}).wait()
    peak = pk_c[0]
    for t in range(1, n_ty):
        peak = jnp.maximum(peak, pk_c[t])
    scale = 1.0 / (p_den + 0.1 * peak[0:1, 0:1])
    own_rows = pl.ds(pl.multiple_of(ty * each, each), each)
    out_probe[0] = probe[0, own_rows, :] + p_re * scale
    out_probe[1] = probe[1, own_rows, :] + p_im * scale


def finish_kernel(tile, probe, out, out_probe, sems):
    copies = [
        pltpu.make_async_copy(tile, out, sems.at[0]),
        pltpu.make_async_copy(probe, out_probe, sems.at[1])]
    for copy in copies:
        copy.start()
    for copy in copies:
        copy.wait()


def table_values(length):
    half = length // 2
    j, m = np.arange(half), np.arange(half)
    even = 2.0 * math.pi / length * (np.outer(2 * m, j) % length)
    odd = 2.0 * math.pi / length * (np.outer(2 * m + 1, j) % length)
    values = []
    for phase in (even, odd, odd.T):
        values += [np.cos(phase) / math.sqrt(length), np.sin(phase) / math.sqrt(length)]
    high = [value.astype(jnp.bfloat16) for value in values]
    low = [(value - h.astype(np.float64)).astype(jnp.bfloat16) for value, h in zip(values, high)]
    return np.stack(high + low)


def body(shape, object_slices, probe_field, positions, live_slots, photon_counts):
    f32 = jnp.float32
    dma = pltpu.SemaphoreType.DMA
    size = probe_field.shape[1]
    half = size // 2
    tile = object_slices[0]
    _, rows, cols = tile.shape
    spots = positions[0, 0, 0].T
    slots = spots.shape[1]
    inner, margin = cols // LANES, half // LANES
    blocks = inner + 2 * margin
    span = size // LANES + 1
    n_ty, n_tx, n_an = shape["ty"], shape["tx"], shape["angle"]
    n_z, each, group = n_ty // 2, size // n_ty, n_an * n_tx
    part = size // n_an
    vmem = pl.BlockSpec(memory_space=pltpu.VMEM)
    smem = pl.BlockSpec(memory_space=pltpu.SMEM)
    hbm = pl.BlockSpec(memory_space=pltpu.HBM)

    def chain_scratch(height):
        return [
            pltpu.VMEM((2, n_z, height, size), f32),
            pltpu.VMEM((n_z, height, size), f32),
            pltpu.VMEM((n_z, height, size), f32),
            pltpu.VMEM((n_an, n_z, height, part), f32),
            pltpu.VMEM((n_z, height, part), f32),
            pltpu.VMEM((n_z, height, part), f32),
            pltpu.VMEM((height, part), f32),
            pltpu.VMEM((group, height, part), f32),
            dma((1,)), dma((1,)), dma((n_an,)), dma((n_an,)), dma((n_z,)), dma((n_z,)), dma((group,)), dma((group,)),
        ]

    new_tile, new_probe = pl.pallas_call(
        functools.partial(step_kernel, shape),
        out_shape=(
            jax.ShapeDtypeStruct((2, rows, cols), f32),
            jax.ShapeDtypeStruct((2, each, size), f32),
        ),
        in_specs=[smem, hbm, hbm, hbm, hbm, hbm],
        out_specs=(vmem, vmem),
        scratch_shapes=[
            pltpu.SMEM(spots.shape, jnp.int32),
            pltpu.VMEM((2, blocks, rows + size, LANES), f32),
            pltpu.VMEM((2, blocks, rows + size, LANES), f32),
            pltpu.VMEM((inner, rows, LANES), f32),
            pltpu.VMEM((slots, 2, span + 2, rows + 2 * size, LANES), f32),
            pltpu.VMEM((9, 8, LANES), jnp.int32),
            pltpu.SMEM((9, 8, LANES), jnp.int32),
            pltpu.VMEM((2, size, size), f32),
            pltpu.VMEM((slots, size // LANES, size, LANES), jnp.int32),
            pltpu.VMEM((slots, size, size), f32),
            pltpu.VMEM((12, half, half), jnp.bfloat16),
            pltpu.VMEM((2, 4, size, size), jnp.bfloat16),
            pltpu.VMEM((slots, 2, size, size), f32),
            pltpu.VMEM((2, 2, inner, half, LANES), f32),
            pltpu.VMEM((2, 2, margin, rows + size, LANES), f32),
            pltpu.VMEM((8, LANES), f32),
            pltpu.VMEM((group, 8, LANES), f32),
            pltpu.VMEM((n_ty, 8, LANES), f32),
            pltpu.VMEM((n_ty, 8, LANES), f32),
            dma((12,)), dma((12,)), dma((9,)), dma((9,)),
            dma((14,)), dma((14,)),
            dma((group,)), dma((group,)), dma((n_ty,)), dma((n_ty,)), dma((n_ty,)), dma((n_ty,)),
            dma((4 + size // LANES,)), dma((inner,)),
            *chain_scratch(each), *chain_scratch(2 * each),
        ],
        compiler_params=pltpu.CompilerParams(
            collective_id=0, has_side_effects=True, vmem_limit_bytes=VMEM_LIMIT),
    )(live_slots[0], *[
        pltpu.with_memory_space_constraint(value, pltpu.HBM)
        for value in (spots, tile, probe_field, photon_counts[0, 0, 0], jnp.asarray(table_values(size)))])

    return pl.pallas_call(
        finish_kernel,
        out_shape=(
            jax.ShapeDtypeStruct(new_tile.shape, f32),
            jax.ShapeDtypeStruct(new_probe.shape, f32),
        ),
        in_specs=[vmem, vmem],
        out_specs=(hbm, hbm),
        scratch_shapes=[dma((2,))],
        compiler_params=pltpu.CompilerParams(vmem_limit_bytes=FINISH_LIMIT),
    )(new_tile, new_probe)


def solution(mesh):
    shape = dict(mesh.shape)

    def step(*args):
        new_tile, new_probe = body(shape, *args)
        return new_tile[None], new_probe

    return jax.shard_map(
        step,
        mesh=mesh,
        in_specs=(
            P("angle", None, "ty", "tx"),
            P(),
            P("angle", "ty", "tx", None, None),
            P("angle", "ty", "tx"),
            P("angle", "ty", "tx", None, None, None),
        ),
        out_specs=(P("angle", None, "ty", "tx"), P(None, "ty", None)),
        check_vma=False,
    )
```

```python
import functools
import math

import jax
import jax.numpy as jnp
import numpy as np
from jax import lax
from jax.experimental import pallas as pl
from jax.experimental.pallas import tpu as pltpu
from jax.sharding import PartitionSpec as P

MESH = pl.DeviceIdType.MESH
LANES = 128
VMEM_LIMIT = 44 * 1024 * 1024
FINISH_LIMIT = 4 * 1024 * 1024
AROUND = tuple((dy, dx) for dy in (-1, 0, 1) for dx in (-1, 0, 1))
BESIDE = tuple(d for d in AROUND if d != (0, 0))
DIAGONALS = tuple(d for d in BESIDE if d[0] and d[1])


def slot_of(dy, dx):
    return (dy + 1) * 3 + dx + 1


def present(dy, dx, shape):
    row = lax.axis_index("ty") + dy
    col = lax.axis_index("tx") + dx
    return (row >= 0) & (row < shape["ty"]) & (col >= 0) & (col < shape["tx"])


def beside_counts(shape):
    found = []
    for axis in ("ty", "tx"):
        at = lax.axis_index(axis)
        found.append(jnp.where(at > 0, 1, 0) + jnp.where(at < shape[axis] - 1, 1, 0))
    return found


def neighbour(dy, dx):
    return {"ty": lax.axis_index("ty") + dy, "tx": lax.axis_index("tx") + dx}


def edge_part(step, size, half):
    return {-1: (half, half), 0: (half, size), 1: (size, half)}[step]


def wide_part(step, size, half):
    return {-1: (0, half), 0: (half, size), 1: (half + size, half)}[step]


def region(ref, rows, blocks):
    return ref.at[:, pl.ds(*blocks), pl.ds(*rows), :]


def split(value):
    high = value.astype(jnp.bfloat16)
    low = (value - high.astype(jnp.float32)).astype(jnp.bfloat16)
    return high, low


def mm(a, b):
    return lax.dot_general(a, b, (((1,), (0,)), ((), ())), preferred_element_type=jnp.float32)


def cat(parts, axis):
    return jnp.concatenate(parts, axis=axis)


def step_kernel(
        shape, live, pos_in, tile_in, probe_in, counts_in, tables_in,
        out, out_probe,
        pos, wide, tot, den, dbuf, metas, smetas, probe, counts, amp, tables, mats,
        xbuf, rim_v, rim_h, pair_h, pk_own, pk_a, pk_b, pk_c,
        hsend, hrecv, nsend, nrecv, fsend, frecv, ksend, krecv, lsend, lrecv, msend, mrecv, local, local_tile,
        *chain_refs):
    f32 = jnp.float32
    size = probe.shape[1]
    half = size // 2
    slots = counts.shape[0]
    rows, cols = tile_in.shape[1], tile_in.shape[2]
    inner = cols // LANES
    margin = half // LANES
    blocks = inner + 2 * margin
    pieces = size // LANES
    span = pieces + 1
    n_ty, n_tx, n_an = shape["ty"], shape["tx"], shape["angle"]
    ty, tx, an = lax.axis_index("ty"), lax.axis_index("tx"), lax.axis_index("angle")
    core, z = ty % 2, ty // 2
    n_z = n_ty // 2
    group = n_an * n_tx
    gid = an * n_tx + tx
    each = size // n_ty
    part = size // n_an
    den_refs, num_refs = chain_refs[:len(chain_refs) // 2], chain_refs[len(chain_refs) // 2:]
    sums_d, sums_n = den_refs[0], num_refs[0]

    load_pos = pltpu.make_async_copy(pos_in, pos, local.at[3])
    load_pos.start()
    load_tile = [
        pltpu.make_async_copy(
            tile_in.at[:, :, pl.ds(j * LANES, LANES)],
            wide.at[:, margin + j, pl.ds(half, rows), :], local_tile.at[j])
        for j in range(inner)]
    load_probe = pltpu.make_async_copy(probe_in, probe, local.at[0])
    load_counts = [
        pltpu.make_async_copy(counts_in.at[:, :, pl.ds(b * LANES, LANES)], counts.at[:, b], local.at[4 + b])
        for b in range(pieces)]
    load_tables = pltpu.make_async_copy(tables_in, tables, local.at[2])
    for copy in load_tile + load_counts + [load_probe, load_tables]:
        copy.start()

    for k in range(9):
        if k != 4:
            metas[k] = jnp.zeros((8, LANES), jnp.int32)
    barrier = pltpu.get_barrier_semaphore()

    def signal(where):
        pl.semaphore_signal(barrier, inc=1, device_id=where, device_id_type=MESH)

    def member(d):
        g = (gid + d) % group
        return g, {"angle": g // n_tx, "tx": g % n_tx}

    for d in range(1, n_ty):
        signal({"ty": (ty + d) % n_ty})
    for d in range(1, group):
        signal(member(d)[1])
    for dy, dx in DIAGONALS:
        @pl.when(present(dy, dx, shape))
        def _():
            signal(neighbour(dy, dx))
    outer_dy, inner_dy = 2 * core - 1, 1 - 2 * core
    outer_there = (ty + outer_dy >= 0) & (ty + outer_dy < n_ty)
    outer_at = pl.multiple_of(core * (half + rows), 8)
    shared_at = pl.multiple_of(half + (1 - core) * (rows - half), 8)
    inner_at = pl.multiple_of((1 - core) * (half + rows), 8)

    def beside(dx):
        return (tx + dx >= 0) & (tx + dx < n_tx)

    load_pos.wait()
    lane8 = lax.broadcasted_iota(jnp.int32, (8, LANES), 1)
    line = jnp.zeros((8, LANES), jnp.int32)
    for s in range(slots):
        line = jnp.where(lane8 == s, pos[0, s], line)
        line = jnp.where(lane8 == slots + s, pos[1, s], line)
    line = jnp.where(lane8 == 2 * slots, live[0, 0], line)
    metas[4] = line

    for copy in load_tile:
        copy.wait()
    n_row, n_col = beside_counts(shape)
    pl.semaphore_wait(barrier, n_ty - 1 + group - 1 + n_row * n_col)

    def rdma(src, dst, s_sem, r_sem, where):
        return pltpu.make_async_remote_copy(
            src_ref=src, dst_ref=dst, send_sem=s_sem, recv_sem=r_sem,
            device_id=where, device_id_type=MESH)

    strips = ((margin, margin), (inner, margin), (2 * margin, inner - 2 * margin))
    SIDES = ((-1, 0), (1, 0), (0, -1), (0, 1))

    def halo_v(dy, i):
        src = region(wide, edge_part(dy, rows, half), strips[i])
        dst = region(wide, wide_part(-dy, rows, half), strips[i])
        k = (dy + 1) // 2 * len(strips) + i
        return rdma(src, dst, hsend.at[k], hrecv.at[k], neighbour(dy, 0))

    def halo_h(dx, dy):
        part_rows = wide_part(dy, rows, half)
        src = region(wide, part_rows, edge_part(dx, inner, margin))
        dst = region(wide, part_rows, wide_part(-dx, inner, margin))
        k = 2 * len(strips) + (dx + 1) // 2 * 3 + dy + 1
        return rdma(src, dst, hsend.at[k], hrecv.at[k], neighbour(0, dx))

    def note(dy, dx):
        k = slot_of(dy, dx)
        return rdma(metas.at[4], metas.at[slot_of(-dy, -dx)], nsend.at[k], nrecv.at[k], neighbour(dy, dx))

    order = sorted(BESIDE, key=lambda d: abs(d[1]))
    for dy, dx in order:
        @pl.when(present(dy, dx, shape))
        def _():
            note(dy, dx).start()
    for dy, dx in SIDES:
        @pl.when(present(dy, dx, shape))
        def _():
            if dx == 0:
                halo_v(dy, 0).start()
                halo_v(dy, 1).start()
            else:
                halo_h(dx, 0).start()
    for dy in (-1, 1):
        @pl.when(present(dy, 0, shape))
        def _():
            halo_v(dy, 2).start()

    @pl.when(jnp.logical_not(outer_there))
    def _():
        rim_v[0] = jnp.zeros(rim_v.shape[1:], f32)

    for side, dx in enumerate((-1, 1)):
        @pl.when(jnp.logical_not(beside(dx)))
        def _():
            rim_h[side] = jnp.zeros(rim_h.shape[1:], f32)

    def clear(n, carry):
        s, ch = n // 2, n % 2
        tall = dbuf.shape[3]
        for b in (0, span + 1):
            dbuf[s, ch, b] = jnp.zeros((tall, LANES), f32)
        for b in range(1, span + 1):
            dbuf[s, ch, b, 0:size, :] = jnp.zeros((size, LANES), f32)
            dbuf[s, ch, b, 2 * size:, :] = jnp.zeros((tall - 2 * size, LANES), f32)
        return carry

    lax.fori_loop(0, 2 * slots, clear, 0)
    den[...] = jnp.zeros_like(den)
    sums_d[...] = jnp.zeros_like(sums_d)
    sums_n[...] = jnp.zeros_like(sums_n)

    load_tables.wait()
    for n in range(2):
        ce, se, co, so, cot, sot = [tables[6 * n + i] for i in range(6)]
        for m, (c, up, down) in enumerate(((ce, se, -se), (co, so, -so), (ce, -se, se), (cot, -sot, sot))):
            mats[n, m, 0:half, 0:half] = c
            mats[n, m, 0:half, half:] = up
            mats[n, m, half:, 0:half] = down
            mats[n, m, half:, half:] = c

    for copy in load_counts:
        copy.wait()
    from_lane = lax.broadcasted_iota(jnp.int32, (size, size), 0)
    to_lane = lax.broadcasted_iota(jnp.int32, (size, size), 1)
    wanted = jnp.where(to_lane < half, 2 * to_lane, 2 * (to_lane - half) + 1)
    shuffle = jnp.where(from_lane == wanted, 1.0, 0.0).astype(jnp.bfloat16)
    shuffle2 = cat([shuffle, shuffle], 0)

    def amplitude(s, carry):
        seen = cat([
            cat([counts[s, b, pl.ds(n, half, stride=2), :] for b in range(pieces)], 1) for n in range(2)], 0).astype(f32)
        amp[s] = 0.05 * jnp.sqrt(mm(cat(list(split(seen)), 1), shuffle2))
        return carry

    lax.fori_loop(0, slots, amplitude, 0)

    load_probe.wait()
    for dy, dx in order:
        @pl.when(present(dy, dx, shape))
        def _():
            note(dy, dx).wait_send()
            note(-dy, -dx).wait_recv()
    for dy in (-1, 1):
        @pl.when(present(dy, 0, shape))
        def _():
            halo_v(-dy, 0).wait_recv()
            halo_v(-dy, 1).wait_recv()
    for dy, dx in DIAGONALS:
        @pl.when(present(dy, dx, shape))
        def _():
            halo_h(dx, dy).start()
    to_scalar = pltpu.make_async_copy(metas, smetas, local.at[3])
    to_scalar.start()
    to_scalar.wait()

    lane = lax.broadcasted_iota(jnp.int32, (size, LANES), 1)

    def spread(piece, shift):
        moved = [pltpu.roll(piece[:, b * LANES:(b + 1) * LANES], shift, axis=1) for b in range(pieces)]
        low = lane[:piece.shape[0]] < shift
        found = [jnp.where(low, 0.0, moved[0])]
        for b in range(1, pieces):
            found.append(jnp.where(low, moved[b - 1], moved[b]))
        found.append(jnp.where(low, moved[-1], 0.0))
        return found

    def spot(k, s):
        return smetas[k, 0, s] - ty * rows + half, smetas[k, 0, slots + s] - tx * cols + half

    far = 64 * LANES

    def place(k, s):
        dy, dx = k // 3 - 1, k % 3 - 1
        row, at = spot(k, s)
        row = jnp.clip(row, dy * rows, dy * rows + rows - 1)
        at = jnp.clip(at, dx * cols, dx * cols + cols - 1)
        first = (at + far * LANES) // LANES - far
        return row, first, (at + far * LANES) % LANES

    power = probe[0] * probe[0] + probe[1] * probe[1]
    base = size

    def gathered(ch, j, start, count, spots):
        total = None
        for s, (row, first, _) in enumerate(spots):
            b = jnp.clip(j - first + 1, 0, span + 1)
            value = dbuf[s, ch, b, pl.ds(start - row + base, count), :]
            total = value if total is None else total + value
        return total

    chunk = half
    for k, (dy, dx) in enumerate(AROUND):
        there = present(dy, dx, shape)
        spots = [place(k, s) for s in range(slots)]

        part_rows = {-1: (half, size), 0: (0, size), 1: (0, half)}[dy]
        for s in range(slots):
            used = there & (s < smetas[k, 0, 2 * slots])
            piece = jnp.where(used, power[part_rows[0]:part_rows[1]], 0.0)
            for b, value in enumerate(spread(piece, spots[s][2])):
                dbuf[s, 0, 1 + b, size + part_rows[0]:size + part_rows[1], :] = value
        tall = range(0, rows, chunk) if dy == 0 else (range(0, half, chunk) if dy < 0 else range(rows - half, rows, chunk))
        if dx == 0:
            def column(j, carry):
                for r in tall:
                    den[j, r:r + chunk, :] += gathered(0, j + margin, half + r, chunk, spots)
                return carry

            lax.fori_loop(0, inner, column, 0)
        else:
            for j in range(margin) if dx < 0 else range(inner - margin, inner):
                for r in tall:
                    den[j, r:r + chunk, :] += gathered(0, j + margin, half + r, chunk, spots)

    def top(value):
        return jnp.max(jnp.max(value, axis=0, keepdims=True), axis=1, keepdims=True)

    pk_own[...] = jnp.broadcast_to(top(jnp.max(den[...], axis=0)), pk_own.shape)
    pk_a[pl.ds(gid, 1)] = pk_own[...][None]
    for d in range(1, group):
        g, where = member(d)
        rdma(pk_own, pk_a.at[gid], ksend.at[d], krecv.at[gid], where).start()

    for dy, dx in SIDES:
        @pl.when(present(dy, dx, shape))
        def _():
            if dx == 0:
                for i in range(len(strips)):
                    halo_v(dy, i).wait_send()
                halo_v(-dy, 2).wait_recv()
            else:
                halo_h(dx, 0).wait_send()
                halo_h(-dx, 0).wait_recv()
    for dy, dx in DIAGONALS:
        @pl.when(present(dy, dx, shape))
        def _():
            halo_h(dx, dy).wait_send()
            halo_h(-dx, dy).wait_recv()

    def matrix(m, axis):
        return cat([mats[0, m], mats[0, m], mats[1, m]], axis)

    def from_left(m, re, im):
        high, low = split(cat([re, im], 0))
        found = mm(matrix(m, 1), cat([high, low, high], 0))
        return found[:half], found[half:]

    def from_right(m, re, im):
        high, low = split(cat([re, im], 1))
        found = mm(cat([high, low, high], 1), matrix(m, 0))
        return found[:, :half], found[:, half:]

    def add_to(total, values):
        cut = total.shape[3]
        length = min(cut, each)
        for t in range(n_ty):
            for ch, value in enumerate(values):
                for i in range(0, each, length):
                    at = ch * each + i
                    total[t % 2, t // 2, at // cut, at % cut:at % cut + length, :] += (
                        value[t * each + i:t * each + i + length, :])

    def extract(s, carry):
        row, first, shift = place(4, s)
        used = s < smetas[4, 0, 2 * slots]
        back = (LANES - shift) % LANES
        keep = lane < LANES - shift
        found = []
        for ch in range(2):
            moved = [
                pltpu.roll(wide[ch, first + b, pl.ds(row, size), :], back, axis=1)
                for b in range(span)]
            found.append(cat([jnp.where(keep, moved[b], moved[b + 1]) for b in range(pieces)], 1))
            xbuf[s, ch] = found[ch]
        add_to(sums_d, (jnp.where(used, found[0] * found[0] + found[1] * found[1], 0.0),))
        return carry

    def slot_steps(s):
        shift = place(4, s)[2]
        used = s < smetas[4, 0, 2 * slots]

        def psi():
            x_re, x_im = xbuf[s, 0], xbuf[s, 1]
            q_re, q_im = probe[0], probe[1]
            return q_re * x_re - q_im * x_im, q_re * x_im + q_im * x_re

        p_re, p_im = psi()
        a = from_left(0, p_re[:half] + p_re[half:], p_im[:half] + p_im[half:])
        b = from_left(1, p_re[:half] - p_re[half:], p_im[:half] - p_im[half:])
        yield
        y_re, y_im = cat([a[0], b[0]], 0), cat([a[1], b[1]], 0)
        a = from_right(2, y_re[:, :half] + y_re[:, half:], y_im[:, :half] + y_im[:, half:])
        b = from_right(3, y_re[:, :half] - y_re[:, half:], y_im[:, :half] - y_im[:, half:])
        yield
        f_re, f_im = cat([a[0], b[0]], 1), cat([a[1], b[1]], 1)
        factor = amp[s] * lax.rsqrt(jnp.maximum(f_re * f_re + f_im * f_im, 0.0625))
        g_re, g_im = f_re * factor, f_im * factor
        a = from_left(2, g_re[:half], g_im[:half])
        b = from_left(3, g_re[half:], g_im[half:])
        yield
        y_re, y_im = cat([a[0] + b[0], a[0] - b[0]], 0), cat([a[1] + b[1], a[1] - b[1]], 0)
        a = from_right(0, y_re[:, :half], y_im[:, :half])
        b = from_right(1, y_re[:, half:], y_im[:, half:])
        yield
        p_re, p_im = psi()
        b_re, b_im = cat([a[0] + b[0], a[0] - b[0]], 1), cat([a[1] + b[1], a[1] - b[1]], 1)
        d_re, d_im = jnp.where(used, b_re - p_re, 0.0), jnp.where(used, b_im - p_im, 0.0)
        x_re, x_im = xbuf[s, 0], xbuf[s, 1]
        q_re, q_im = probe[0], probe[1]
        for ch, value in enumerate((q_re * d_re + q_im * d_im, q_re * d_im - q_im * d_re)):
            for i, moved in enumerate(spread(value, shift)):
                dbuf[s, ch, 1 + i, size:2 * size, :] = moved
        add_to(sums_n, (x_re * d_re + x_im * d_im, x_re * d_im - x_im * d_re))
        yield

    class Chain:
        def __init__(self, refs):
            (self.sums, self.r1, self.s1, self.r2, self.s2, self.r3, self.s3, self.g4,
             self.send1, self.recv1, self.send2, self.recv2, self.send3, self.recv3, self.send4, self.recv4) = refs

        def pair(self):
            return rdma(self.sums.at[1 - core], self.r1, self.send1.at[0], self.recv1.at[0], {"ty": ty + 1 - 2 * core})

        def over_plane(self, d, get):
            g, where = member(d)
            at = g if get else gid
            lanes = pl.ds(pl.multiple_of(g // n_tx * part, part), part)
            return rdma(
                self.s1.at[:, g % n_tx, :, lanes], self.r2.at[at], self.send2.at[d], self.recv2.at[at], where)

        def over_z(self, d, get):
            o = (z + d) % n_z
            at = o if get else z
            return rdma(self.s2.at[o], self.r3.at[at], self.send3.at[d], self.recv3.at[at], {"ty": o * 2 + core})

        def over_group(self, d, get):
            g, where = member(d)
            at = g if get else gid
            return rdma(self.s3, self.g4.at[at], self.send4.at[d], self.recv4.at[at], where)

        def step1(self):
            self.pair().start()

        def step2(self):
            self.pair().wait()
            self.s1[...] = self.sums[core] + self.r1[...]
            for d in range(1, group):
                self.over_plane(d, False).start()

        def step3(self):
            for d in range(1, group):
                self.over_plane(d, True).wait()
            total = self.s1[:, tx, :, pl.ds(pl.multiple_of(an * part, part), part)]
            for d in range(1, group):
                total = total + self.r2[(gid + d) % group]
            self.s2[...] = total
            for d in range(1, n_z):
                self.over_z(d, False).start()

        def step4(self):
            for d in range(1, n_z):
                self.over_z(d, True).wait()
            total = self.s2[z]
            for d in range(1, n_z):
                total = total + self.r3[(z + d) % n_z]
            self.s3[...] = total
            self.g4[pl.ds(gid, 1)] = total[None]
            for d in range(1, group):
                self.over_group(d, False).start()

        def result(self):
            for d in range(1, group):
                self.over_group(d, True).wait()
            return cat([cat([self.g4[a * n_tx + t] for t in range(n_tx)], 0) for a in range(n_an)], 1)

    den_chain, num_chain = Chain(den_refs), Chain(num_refs)

    def some_slots(*which):
        running = [slot_steps(s) for s in which]
        for _ in range(5):
            for steps in running:
                next(steps)

    lax.fori_loop(0, slots, extract, 0)
    den_chain.step1()
    some_slots(*range(slots // 2))
    den_chain.step2()
    some_slots(*range(slots // 2, slots))
    num_chain.step1()
    for d in range(1, group):
        g, where = member(d)
        rdma(pk_own, pk_a.at[g], ksend.at[d], krecv.at[g], where).wait()
    peak = pk_a[0]
    for g in range(1, group):
        peak = jnp.maximum(peak, pk_a[g])
    pk_b[pl.ds(ty, 1)] = peak[None]
    for d in range(1, n_ty):
        rdma(pk_b.at[ty], pk_b.at[ty], lsend.at[d], lrecv.at[ty], {"ty": (ty + d) % n_ty}).start()
    spots = [place(4, s) for s in range(slots)]
    def total_at(start, count, lowest, number):
        def column(n, carry):
            j = lowest + n // 2
            ch = n % 2
            for r in range(0, count, chunk):
                at = start + r if isinstance(start, int) else pl.multiple_of(start + r, 8)
                tot[ch, j, pl.ds(at, chunk), :] = gathered(ch, j, at, chunk, spots)
            return carry

        lax.fori_loop(0, 2 * number, column, 0)

    middle = inner - 2 * margin
    third = middle // 3
    groups = (
        (2 * margin, third), (2 * margin + third, third), (2 * margin + 2 * third, middle - 2 * third),
        (margin, margin), (inner, margin))

    def fold_outer(i):
        start, count = groups[i]
        return rdma(
            region(tot, (outer_at, half), groups[i]), rim_v.at[0, :, pl.ds(start - margin, count)],
            fsend.at[i], frecv.at[i], {"ty": ty + outer_dy})

    def fold_inner():
        return rdma(
            region(tot, (inner_at, half), (margin, inner)), rim_v.at[1], fsend.at[13], frecv.at[13], {"ty": ty + inner_dy})

    def side_of(dx):
        return wide_part(dx, inner, margin)

    def fold_beside(dx, n):
        k = 5 + (dx + 1) // 2 + 6 * n
        start = shared_at if n else pl.multiple_of(half + core * half, 8)
        count = half if n else rows - half
        return rdma(
            region(tot, (start, count), side_of(dx)),
            rim_h.at[(1 - dx) // 2, :, :, pl.ds(pl.multiple_of(start - half, 8), count)],
            fsend.at[k], frecv.at[k], {"tx": tx + dx})

    def fold_corner(dx):
        k = 7 + (dx + 1) // 2
        return rdma(
            region(tot, (outer_at, half), side_of(dx)), rim_h.at[(1 - dx) // 2, :, :, pl.ds(rows, half)],
            fsend.at[k], frecv.at[k], {"tx": tx + dx})

    def fold_pair(dx):
        k = 9 + (dx + 1) // 2
        return rdma(
            region(tot, (inner_at, half), side_of(dx)), pair_h.at[(dx + 1) // 2],
            fsend.at[k], frecv.at[k], {"ty": ty + inner_dy})

    @pl.when(outer_there)
    def _():
        total_at(outer_at, half, *groups[0])
        fold_outer(0).start()

    for dx in (-1, 1):
        @pl.when(beside(dx))
        def _():
            total_at(inner_at, half, *side_of(dx))
            fold_pair(dx).start()
            total_at(outer_at, half, *side_of(dx))
            total_at(half, rows, *side_of(dx))
    num_chain.step2()
    for dx in (-1, 1):
        @pl.when(beside(dx) & outer_there)
        def _():
            fold_corner(dx).start()
    den_chain.step3()
    @pl.when(outer_there)
    def _():
        total_at(outer_at, half, *groups[1])
        fold_outer(1).start()
        for i in (2, 3, 4):
            total_at(outer_at, half, *groups[i])

    total_at(inner_at, half, margin, inner)
    fold_inner().start()
    total_at(half, rows, margin, inner)
    num_chain.step3()

    @pl.when(outer_there)
    def _():
        fold_outer(2).start()

    den_chain.step4()
    for dx in (-1, 1):
        @pl.when(beside(dx))
        def _():
            fold_beside(dx, 0).start()
    for dx in (-1, 1):
        @pl.when(beside(dx) & outer_there)
        def _():
            fold_corner(-dx).wait_recv()
            start, count = edge_part(dx, inner, margin)
            tot[:, pl.ds(start, count), pl.ds(outer_at, half), :] += rim_h[(dx + 1) // 2, :, :, rows:, :]

    @pl.when(outer_there)
    def _():
        fold_outer(3).start()
        fold_outer(4).start()

    p_den = den_chain.result()
    pk_c[pl.ds(ty, 1)] = jnp.broadcast_to(top(p_den), pk_own.shape)[None]
    for d in range(1, n_ty):
        rdma(pk_c.at[ty], pk_c.at[ty], msend.at[d], mrecv.at[ty], {"ty": (ty + d) % n_ty}).start()
    num_chain.step4()
    for dx in (-1, 1):
        @pl.when(beside(dx))
        def _():
            fold_pair(dx).wait()
            tot[:, pl.ds(*side_of(dx)), pl.ds(shared_at, half), :] += pair_h[(dx + 1) // 2]
            fold_beside(dx, 1).start()
    full = num_chain.result()
    p_re, p_im = full[:each], full[each:]

    for dx in (-1, 1):
        @pl.when(beside(dx))
        def _():
            for n in range(2):
                fold_beside(dx, n).wait_send()
                fold_beside(-dx, n).wait_recv()

        @pl.when(beside(dx) & outer_there)
        def _():
            fold_corner(dx).wait_send()

    @pl.when(outer_there)
    def _():
        for i in range(len(groups)):
            fold_outer(i).wait()

    fold_inner().wait()
    for d in range(1, n_ty):
        o = (ty + d) % n_ty
        rdma(pk_b.at[ty], pk_b.at[o], lsend.at[d], lrecv.at[o], {"ty": o}).wait()
    peak = pk_b[0]
    for t in range(1, n_ty):
        peak = jnp.maximum(peak, pk_b[t])
    den[...] = 1.0 / (den[...] + 0.1 * peak[0:1, 0:1])

    for j in range(inner):
        for ch in range(2):
            for r in range(0, rows, chunk):
                inside = slice(half + r, half + r + chunk)
                value = tot[ch, j + margin, inside, :]
                if r < half:
                    value = value + rim_v[core, ch, j, r:r + chunk, :]
                if r >= rows - half:
                    value = value + rim_v[1 - core, ch, j, r - rows + half:r - rows + half + chunk, :]
                if j < margin:
                    value = value + rim_h[0, ch, j, r:r + chunk, :]
                if j >= inner - margin:
                    value = value + rim_h[1, ch, j - inner + margin, r:r + chunk, :]
                own = wide[ch, j + margin, inside, :]
                out[ch, r:r + chunk, j * LANES:(j + 1) * LANES] = own + value * den[j, r:r + chunk, :]

    for d in range(1, n_ty):
        o = (ty + d) % n_ty
        rdma(pk_c.at[ty], pk_c.at[o], msend.at[d], mrecv.at[o], {"ty": o}).wait()
    peak = pk_c[0]
    for t in range(1, n_ty):
        peak = jnp.maximum(peak, pk_c[t])
    scale = 1.0 / (p_den + 0.1 * peak[0:1, 0:1])
    own_rows = pl.ds(pl.multiple_of(ty * each, each), each)
    out_probe[0] = probe[0, own_rows, :] + p_re * scale
    out_probe[1] = probe[1, own_rows, :] + p_im * scale


def finish_kernel(tile, probe, out, out_probe, sems):
    copies = [
        pltpu.make_async_copy(tile, out, sems.at[0]),
        pltpu.make_async_copy(probe, out_probe, sems.at[1])]
    for copy in copies:
        copy.start()
    for copy in copies:
        copy.wait()


def table_values(length):
    half = length // 2
    j, m = np.arange(half), np.arange(half)
    even = 2.0 * math.pi / length * (np.outer(2 * m, j) % length)
    odd = 2.0 * math.pi / length * (np.outer(2 * m + 1, j) % length)
    values = []
    for phase in (even, odd, odd.T):
        values += [np.cos(phase) / math.sqrt(length), np.sin(phase) / math.sqrt(length)]
    high = [value.astype(jnp.bfloat16) for value in values]
    low = [(value - h.astype(np.float64)).astype(jnp.bfloat16) for value, h in zip(values, high)]
    return np.stack(high + low)


def body(shape, object_slices, probe_field, positions, live_slots, photon_counts):
    f32 = jnp.float32
    dma = pltpu.SemaphoreType.DMA
    size = probe_field.shape[1]
    half = size // 2
    tile = object_slices[0]
    _, rows, cols = tile.shape
    spots = positions[0, 0, 0].T
    slots = spots.shape[1]
    inner, margin = cols // LANES, half // LANES
    blocks = inner + 2 * margin
    span = size // LANES + 1
    n_ty, n_tx, n_an = shape["ty"], shape["tx"], shape["angle"]
    n_z, each, group = n_ty // 2, size // n_ty, n_an * n_tx
    part = size // n_an
    vmem = pl.BlockSpec(memory_space=pltpu.VMEM)
    smem = pl.BlockSpec(memory_space=pltpu.SMEM)
    hbm = pl.BlockSpec(memory_space=pltpu.HBM)

    def chain_scratch(height):
        cut = height // n_tx
        return [
            pltpu.VMEM((2, n_z, n_tx, cut, size), f32),
            pltpu.VMEM((n_z, n_tx, cut, size), f32),
            pltpu.VMEM((n_z, n_tx, cut, size), f32),
            pltpu.VMEM((group, n_z, cut, part), f32),
            pltpu.VMEM((n_z, cut, part), f32),
            pltpu.VMEM((n_z, cut, part), f32),
            pltpu.VMEM((cut, part), f32),
            pltpu.VMEM((group, cut, part), f32),
            dma((1,)), dma((1,)), dma((group,)), dma((group,)), dma((n_z,)), dma((n_z,)), dma((group,)), dma((group,)),
        ]

    new_tile, new_probe = pl.pallas_call(
        functools.partial(step_kernel, shape),
        out_shape=(
            jax.ShapeDtypeStruct((2, rows, cols), f32),
            jax.ShapeDtypeStruct((2, each, size), f32),
        ),
        in_specs=[smem, hbm, hbm, hbm, hbm, hbm],
        out_specs=(vmem, vmem),
        scratch_shapes=[
            pltpu.SMEM(spots.shape, jnp.int32),
            pltpu.VMEM((2, blocks, rows + size, LANES), f32),
            pltpu.VMEM((2, blocks, rows + size, LANES), f32),
            pltpu.VMEM((inner, rows, LANES), f32),
            pltpu.VMEM((slots, 2, span + 2, rows + 2 * size, LANES), f32),
            pltpu.VMEM((9, 8, LANES), jnp.int32),
            pltpu.SMEM((9, 8, LANES), jnp.int32),
            pltpu.VMEM((2, size, size), f32),
            pltpu.VMEM((slots, size // LANES, size, LANES), jnp.int32),
            pltpu.VMEM((slots, size, size), f32),
            pltpu.VMEM((12, half, half), jnp.bfloat16),
            pltpu.VMEM((2, 4, size, size), jnp.bfloat16),
            pltpu.VMEM((slots, 2, size, size), f32),
            pltpu.VMEM((2, 2, inner, half, LANES), f32),
            pltpu.VMEM((2, 2, margin, rows + half, LANES), f32),
            pltpu.VMEM((2, 2, margin, half, LANES), f32),
            pltpu.VMEM((8, LANES), f32),
            pltpu.VMEM((group, 8, LANES), f32),
            pltpu.VMEM((n_ty, 8, LANES), f32),
            pltpu.VMEM((n_ty, 8, LANES), f32),
            dma((12,)), dma((12,)), dma((9,)), dma((9,)),
            dma((14,)), dma((14,)),
            dma((group,)), dma((group,)), dma((n_ty,)), dma((n_ty,)), dma((n_ty,)), dma((n_ty,)),
            dma((4 + size // LANES,)), dma((inner,)),
            *chain_scratch(each), *chain_scratch(2 * each),
        ],
        compiler_params=pltpu.CompilerParams(
            collective_id=0, has_side_effects=True, vmem_limit_bytes=VMEM_LIMIT),
    )(live_slots[0], *[
        pltpu.with_memory_space_constraint(value, pltpu.HBM)
        for value in (spots, tile, probe_field, photon_counts[0, 0, 0], jnp.asarray(table_values(size)))])

    return pl.pallas_call(
        finish_kernel,
        out_shape=(
            jax.ShapeDtypeStruct(new_tile.shape, f32),
            jax.ShapeDtypeStruct(new_probe.shape, f32),
        ),
        in_specs=[vmem, vmem],
        out_specs=(hbm, hbm),
        scratch_shapes=[dma((2,))],
        compiler_params=pltpu.CompilerParams(vmem_limit_bytes=FINISH_LIMIT),
    )(new_tile, new_probe)


def solution(mesh):
    shape = dict(mesh.shape)

    def step(*args):
        new_tile, new_probe = body(shape, *args)
        return new_tile[None], new_probe

    return jax.shard_map(
        step,
        mesh=mesh,
        in_specs=(
            P("angle", None, "ty", "tx"),
            P(),
            P("angle", "ty", "tx", None, None),
            P("angle", "ty", "tx"),
            P("angle", "ty", "tx", None, None, None),
        ),
        out_specs=(P("angle", None, "ty", "tx"), P(None, "ty", None)),
        check_vma=False,
    )
```

```python
import functools
import math

import jax
import jax.numpy as jnp
import numpy as np
from jax import lax
from jax.experimental import pallas as pl
from jax.experimental.pallas import tpu as pltpu
from jax.sharding import PartitionSpec as P

MESH = pl.DeviceIdType.MESH
LANES = 128
VMEM_LIMIT = 40 * 1024 * 1024
FINISH_LIMIT = 4 * 1024 * 1024
AROUND = tuple((dy, dx) for dy in (-1, 0, 1) for dx in (-1, 0, 1))
BESIDE = tuple(d for d in AROUND if d != (0, 0))
DIAGONALS = tuple(d for d in BESIDE if d[0] and d[1])


def slot_of(dy, dx):
    return (dy + 1) * 3 + dx + 1


def present(dy, dx, shape):
    row = lax.axis_index("ty") + dy
    col = lax.axis_index("tx") + dx
    return (row >= 0) & (row < shape["ty"]) & (col >= 0) & (col < shape["tx"])


def beside_counts(shape):
    found = []
    for axis in ("ty", "tx"):
        at = lax.axis_index(axis)
        found.append(jnp.where(at > 0, 1, 0) + jnp.where(at < shape[axis] - 1, 1, 0))
    return found


def neighbour(dy, dx):
    return {"ty": lax.axis_index("ty") + dy, "tx": lax.axis_index("tx") + dx}


def edge_part(step, size, half):
    return {-1: (half, half), 0: (half, size), 1: (size, half)}[step]


def wide_part(step, size, half):
    return {-1: (0, half), 0: (half, size), 1: (half + size, half)}[step]


def region(ref, rows, blocks):
    return ref.at[:, pl.ds(*blocks), pl.ds(*rows), :]


def split(value):
    high = value.astype(jnp.bfloat16)
    low = (value - high.astype(jnp.float32)).astype(jnp.bfloat16)
    return high, low


def mm(a, b):
    return lax.dot_general(a, b, (((1,), (0,)), ((), ())), preferred_element_type=jnp.float32)


def cat(parts, axis):
    return jnp.concatenate(parts, axis=axis)


def step_kernel(
        shape, live, pos_in, tile_in, probe_in, counts_in, tables_in,
        wide, tot, den, rim_v, rim_h, out_probe,
        pos, dbuf, metas, smetas, probe, counts, amp, tables, mats,
        xbuf, pair_h, pk_own, pk_a, pk_b, pk_c,
        hsend, hrecv, nsend, nrecv, fsend, frecv, ksend, krecv, lsend, lrecv, msend, mrecv, local, local_tile,
        *chain_refs):
    f32 = jnp.float32
    size = probe.shape[1]
    half = size // 2
    slots = counts.shape[0]
    rows, cols = tile_in.shape[1], tile_in.shape[2]
    inner = cols // LANES
    margin = half // LANES
    blocks = inner + 2 * margin
    pieces = size // LANES
    span = pieces + 1
    n_ty, n_tx, n_an = shape["ty"], shape["tx"], shape["angle"]
    ty, tx, an = lax.axis_index("ty"), lax.axis_index("tx"), lax.axis_index("angle")
    core, z = ty % 2, ty // 2
    n_z = n_ty // 2
    group = n_an * n_tx
    gid = an * n_tx + tx
    each = size // n_ty
    part = size // n_an
    den_refs, num_refs = chain_refs[:len(chain_refs) // 2], chain_refs[len(chain_refs) // 2:]
    sums_d, sums_n = den_refs[0], num_refs[0]

    load_pos = pltpu.make_async_copy(pos_in, pos, local.at[3])
    load_pos.start()
    load_tile = [
        pltpu.make_async_copy(
            tile_in.at[:, :, pl.ds(j * LANES, LANES)],
            wide.at[:, margin + j, pl.ds(half, rows), :], local_tile.at[j])
        for j in range(inner)]
    load_probe = pltpu.make_async_copy(probe_in, probe, local.at[0])
    load_counts = [
        pltpu.make_async_copy(counts_in.at[:, :, pl.ds(b * LANES, LANES)], counts.at[:, b], local.at[4 + b])
        for b in range(pieces)]
    load_tables = pltpu.make_async_copy(tables_in, tables, local.at[2])
    for copy in load_tile + load_counts + [load_probe, load_tables]:
        copy.start()

    for k in range(9):
        if k != 4:
            metas[k] = jnp.zeros((8, LANES), jnp.int32)
    barrier = pltpu.get_barrier_semaphore()

    def signal(where):
        pl.semaphore_signal(barrier, inc=1, device_id=where, device_id_type=MESH)

    def member(d):
        g = (gid + d) % group
        return g, {"angle": g // n_tx, "tx": g % n_tx}

    for d in range(1, n_ty):
        signal({"ty": (ty + d) % n_ty})
    for d in range(1, group):
        signal(member(d)[1])
    for dy, dx in DIAGONALS:
        @pl.when(present(dy, dx, shape))
        def _():
            signal(neighbour(dy, dx))
    outer_dy, inner_dy = 2 * core - 1, 1 - 2 * core
    outer_there = (ty + outer_dy >= 0) & (ty + outer_dy < n_ty)
    outer_at = pl.multiple_of(core * (half + rows), 8)
    shared_at = pl.multiple_of(half + (1 - core) * (rows - half), 8)
    inner_at = pl.multiple_of((1 - core) * (half + rows), 8)

    def beside(dx):
        return (tx + dx >= 0) & (tx + dx < n_tx)

    load_pos.wait()
    lane8 = lax.broadcasted_iota(jnp.int32, (8, LANES), 1)
    line = jnp.zeros((8, LANES), jnp.int32)
    for s in range(slots):
        line = jnp.where(lane8 == s, pos[0, s], line)
        line = jnp.where(lane8 == slots + s, pos[1, s], line)
    line = jnp.where(lane8 == 2 * slots, live[0, 0], line)
    metas[4] = line

    for copy in load_tile:
        copy.wait()
    n_row, n_col = beside_counts(shape)
    pl.semaphore_wait(barrier, n_ty - 1 + group - 1 + n_row * n_col)

    def rdma(src, dst, s_sem, r_sem, where):
        return pltpu.make_async_remote_copy(
            src_ref=src, dst_ref=dst, send_sem=s_sem, recv_sem=r_sem,
            device_id=where, device_id_type=MESH)

    strips = ((margin, margin), (inner, margin), (2 * margin, inner - 2 * margin))
    SIDES = ((-1, 0), (1, 0), (0, -1), (0, 1))

    def halo_v(dy, i):
        src = region(wide, edge_part(dy, rows, half), strips[i])
        dst = region(wide, wide_part(-dy, rows, half), strips[i])
        k = (dy + 1) // 2 * len(strips) + i
        return rdma(src, dst, hsend.at[k], hrecv.at[k], neighbour(dy, 0))

    def halo_h(dx, dy):
        part_rows = wide_part(dy, rows, half)
        src = region(wide, part_rows, edge_part(dx, inner, margin))
        dst = region(wide, part_rows, wide_part(-dx, inner, margin))
        k = 2 * len(strips) + (dx + 1) // 2 * 3 + dy + 1
        return rdma(src, dst, hsend.at[k], hrecv.at[k], neighbour(0, dx))

    def note(dy, dx):
        k = slot_of(dy, dx)
        return rdma(metas.at[4], metas.at[slot_of(-dy, -dx)], nsend.at[k], nrecv.at[k], neighbour(dy, dx))

    order = sorted(BESIDE, key=lambda d: abs(d[1]))
    for dy, dx in order:
        @pl.when(present(dy, dx, shape))
        def _():
            note(dy, dx).start()
    for dy, dx in SIDES:
        @pl.when(present(dy, dx, shape))
        def _():
            if dx == 0:
                halo_v(dy, 0).start()
                halo_v(dy, 1).start()
            else:
                halo_h(dx, 0).start()
    for dy in (-1, 1):
        @pl.when(present(dy, 0, shape))
        def _():
            halo_v(dy, 2).start()

    @pl.when(jnp.logical_not(outer_there))
    def _():
        rim_v[0] = jnp.zeros(rim_v.shape[1:], f32)

    for side, dx in enumerate((-1, 1)):
        @pl.when(jnp.logical_not(beside(dx)))
        def _():
            rim_h[side] = jnp.zeros(rim_h.shape[1:], f32)

    def clear(n, carry):
        s, ch = n // 2, n % 2
        tall = dbuf.shape[3]
        for b in (0, span + 1):
            dbuf[s, ch, b] = jnp.zeros((tall, LANES), f32)
        for b in range(1, span + 1):
            dbuf[s, ch, b, 0:size, :] = jnp.zeros((size, LANES), f32)
            dbuf[s, ch, b, 2 * size:, :] = jnp.zeros((tall - 2 * size, LANES), f32)
        return carry

    lax.fori_loop(0, 2 * slots, clear, 0)
    den[...] = jnp.zeros_like(den)
    sums_d[...] = jnp.zeros_like(sums_d)
    sums_n[...] = jnp.zeros_like(sums_n)

    load_tables.wait()
    for n in range(2):
        ce, se, co, so, cot, sot = [tables[6 * n + i] for i in range(6)]
        for m, (c, up, down) in enumerate(((ce, se, -se), (co, so, -so), (ce, -se, se), (cot, -sot, sot))):
            mats[n, m, 0:half, 0:half] = c
            mats[n, m, 0:half, half:] = up
            mats[n, m, half:, 0:half] = down
            mats[n, m, half:, half:] = c

    for copy in load_counts:
        copy.wait()
    from_lane = lax.broadcasted_iota(jnp.int32, (size, size), 0)
    to_lane = lax.broadcasted_iota(jnp.int32, (size, size), 1)
    wanted = jnp.where(to_lane < half, 2 * to_lane, 2 * (to_lane - half) + 1)
    shuffle = jnp.where(from_lane == wanted, 1.0, 0.0).astype(jnp.bfloat16)
    shuffle2 = cat([shuffle, shuffle], 0)

    def amplitude(s, carry):
        seen = cat([
            cat([counts[s, b, pl.ds(n, half, stride=2), :] for b in range(pieces)], 1) for n in range(2)], 0).astype(f32)
        amp[s] = 0.05 * jnp.sqrt(mm(cat(list(split(seen)), 1), shuffle2))
        return carry

    lax.fori_loop(0, slots, amplitude, 0)

    load_probe.wait()
    for dy, dx in order:
        @pl.when(present(dy, dx, shape))
        def _():
            note(dy, dx).wait_send()
            note(-dy, -dx).wait_recv()
    for dy in (-1, 1):
        @pl.when(present(dy, 0, shape))
        def _():
            halo_v(-dy, 0).wait_recv()
            halo_v(-dy, 1).wait_recv()
    for dy, dx in DIAGONALS:
        @pl.when(present(dy, dx, shape))
        def _():
            halo_h(dx, dy).start()
    to_scalar = pltpu.make_async_copy(metas, smetas, local.at[3])
    to_scalar.start()
    to_scalar.wait()

    lane = lax.broadcasted_iota(jnp.int32, (size, LANES), 1)

    def spread(piece, shift):
        moved = [pltpu.roll(piece[:, b * LANES:(b + 1) * LANES], shift, axis=1) for b in range(pieces)]
        low = lane[:piece.shape[0]] < shift
        found = [jnp.where(low, 0.0, moved[0])]
        for b in range(1, pieces):
            found.append(jnp.where(low, moved[b - 1], moved[b]))
        found.append(jnp.where(low, moved[-1], 0.0))
        return found

    def spot(k, s):
        return smetas[k, 0, s] - ty * rows + half, smetas[k, 0, slots + s] - tx * cols + half

    far = 64 * LANES

    def place(k, s):
        dy, dx = k // 3 - 1, k % 3 - 1
        row, at = spot(k, s)
        row = jnp.clip(row, dy * rows, dy * rows + rows - 1)
        at = jnp.clip(at, dx * cols, dx * cols + cols - 1)
        first = (at + far * LANES) // LANES - far
        return row, first, (at + far * LANES) % LANES

    power = probe[0] * probe[0] + probe[1] * probe[1]
    base = size

    def gathered(ch, j, start, count, spots):
        total = None
        for s, (row, first, _) in enumerate(spots):
            b = jnp.clip(j - first + 1, 0, span + 1)
            value = dbuf[s, ch, b, pl.ds(start - row + base, count), :]
            total = value if total is None else total + value
        return total

    chunk = half
    for k, (dy, dx) in enumerate(AROUND):
        there = present(dy, dx, shape)
        spots = [place(k, s) for s in range(slots)]

        part_rows = {-1: (half, size), 0: (0, size), 1: (0, half)}[dy]
        for s in range(slots):
            used = there & (s < smetas[k, 0, 2 * slots])
            piece = jnp.where(used, power[part_rows[0]:part_rows[1]], 0.0)
            for b, value in enumerate(spread(piece, spots[s][2])):
                dbuf[s, 0, 1 + b, size + part_rows[0]:size + part_rows[1], :] = value
        tall = range(0, rows, chunk) if dy == 0 else (range(0, half, chunk) if dy < 0 else range(rows - half, rows, chunk))
        if dx == 0:
            def column(j, carry):
                for r in tall:
                    den[j, r:r + chunk, :] += gathered(0, j + margin, half + r, chunk, spots)
                return carry

            lax.fori_loop(0, inner, column, 0)
        else:
            for j in range(margin) if dx < 0 else range(inner - margin, inner):
                for r in tall:
                    den[j, r:r + chunk, :] += gathered(0, j + margin, half + r, chunk, spots)

    def top(value):
        return jnp.max(jnp.max(value, axis=0, keepdims=True), axis=1, keepdims=True)

    pk_own[...] = jnp.broadcast_to(top(jnp.max(den[...], axis=0)), pk_own.shape)
    pk_a[pl.ds(gid, 1)] = pk_own[...][None]
    for d in range(1, group):
        g, where = member(d)
        rdma(pk_own, pk_a.at[gid], ksend.at[d], krecv.at[gid], where).start()

    for dy, dx in SIDES:
        @pl.when(present(dy, dx, shape))
        def _():
            if dx == 0:
                for i in range(len(strips)):
                    halo_v(dy, i).wait_send()
                halo_v(-dy, 2).wait_recv()
            else:
                halo_h(dx, 0).wait_send()
                halo_h(-dx, 0).wait_recv()
    for dy, dx in DIAGONALS:
        @pl.when(present(dy, dx, shape))
        def _():
            halo_h(dx, dy).wait_send()
            halo_h(-dx, dy).wait_recv()

    def matrix(m, axis):
        return cat([mats[0, m], mats[0, m], mats[1, m]], axis)

    def from_left(m, re, im):
        high, low = split(cat([re, im], 0))
        found = mm(matrix(m, 1), cat([high, low, high], 0))
        return found[:half], found[half:]

    def from_right(m, re, im):
        high, low = split(cat([re, im], 1))
        found = mm(cat([high, low, high], 1), matrix(m, 0))
        return found[:, :half], found[:, half:]

    def add_to(total, values):
        cut = total.shape[3]
        length = min(cut, each)
        for t in range(n_ty):
            for ch, value in enumerate(values):
                for i in range(0, each, length):
                    at = ch * each + i
                    total[t % 2, t // 2, at // cut, at % cut:at % cut + length, :] += (
                        value[t * each + i:t * each + i + length, :])

    def extract(s, carry):
        row, first, shift = place(4, s)
        used = s < smetas[4, 0, 2 * slots]
        back = (LANES - shift) % LANES
        keep = lane < LANES - shift
        found = []
        for ch in range(2):
            moved = [
                pltpu.roll(wide[ch, first + b, pl.ds(row, size), :], back, axis=1)
                for b in range(span)]
            found.append(cat([jnp.where(keep, moved[b], moved[b + 1]) for b in range(pieces)], 1))
            xbuf[s, ch] = found[ch]
        add_to(sums_d, (jnp.where(used, found[0] * found[0] + found[1] * found[1], 0.0),))
        return carry

    def slot_steps(s):
        shift = place(4, s)[2]
        used = s < smetas[4, 0, 2 * slots]

        def psi():
            x_re, x_im = xbuf[s, 0], xbuf[s, 1]
            q_re, q_im = probe[0], probe[1]
            return q_re * x_re - q_im * x_im, q_re * x_im + q_im * x_re

        p_re, p_im = psi()
        a = from_left(0, p_re[:half] + p_re[half:], p_im[:half] + p_im[half:])
        b = from_left(1, p_re[:half] - p_re[half:], p_im[:half] - p_im[half:])
        yield
        y_re, y_im = cat([a[0], b[0]], 0), cat([a[1], b[1]], 0)
        a = from_right(2, y_re[:, :half] + y_re[:, half:], y_im[:, :half] + y_im[:, half:])
        b = from_right(3, y_re[:, :half] - y_re[:, half:], y_im[:, :half] - y_im[:, half:])
        yield
        f_re, f_im = cat([a[0], b[0]], 1), cat([a[1], b[1]], 1)
        factor = amp[s] * lax.rsqrt(jnp.maximum(f_re * f_re + f_im * f_im, 0.0625))
        g_re, g_im = f_re * factor, f_im * factor
        a = from_left(2, g_re[:half], g_im[:half])
        b = from_left(3, g_re[half:], g_im[half:])
        yield
        y_re, y_im = cat([a[0] + b[0], a[0] - b[0]], 0), cat([a[1] + b[1], a[1] - b[1]], 0)
        a = from_right(0, y_re[:, :half], y_im[:, :half])
        b = from_right(1, y_re[:, half:], y_im[:, half:])
        yield
        p_re, p_im = psi()
        b_re, b_im = cat([a[0] + b[0], a[0] - b[0]], 1), cat([a[1] + b[1], a[1] - b[1]], 1)
        d_re, d_im = jnp.where(used, b_re - p_re, 0.0), jnp.where(used, b_im - p_im, 0.0)
        x_re, x_im = xbuf[s, 0], xbuf[s, 1]
        q_re, q_im = probe[0], probe[1]
        for ch, value in enumerate((q_re * d_re + q_im * d_im, q_re * d_im - q_im * d_re)):
            for i, moved in enumerate(spread(value, shift)):
                dbuf[s, ch, 1 + i, size:2 * size, :] = moved
        add_to(sums_n, (x_re * d_re + x_im * d_im, x_re * d_im - x_im * d_re))
        yield

    class Chain:
        def __init__(self, refs):
            (self.sums, self.r1, self.s1, self.r2, self.s2, self.r3, self.s3, self.g4,
             self.send1, self.recv1, self.send2, self.recv2, self.send3, self.recv3, self.send4, self.recv4) = refs

        def pair(self):
            return rdma(self.sums.at[1 - core], self.r1, self.send1.at[0], self.recv1.at[0], {"ty": ty + 1 - 2 * core})

        def over_plane(self, d, get):
            g, where = member(d)
            at = g if get else gid
            lanes = pl.ds(pl.multiple_of(g // n_tx * part, part), part)
            return rdma(
                self.s1.at[:, g % n_tx, :, lanes], self.r2.at[at], self.send2.at[d], self.recv2.at[at], where)

        def over_z(self, d, get):
            o = (z + d) % n_z
            at = o if get else z
            return rdma(self.s2.at[o], self.r3.at[at], self.send3.at[d], self.recv3.at[at], {"ty": o * 2 + core})

        def over_group(self, d, get):
            g, where = member(d)
            at = g if get else gid
            return rdma(self.s3, self.g4.at[at], self.send4.at[d], self.recv4.at[at], where)

        def step1(self):
            self.pair().start()

        def step2(self):
            self.pair().wait()
            self.s1[...] = self.sums[core] + self.r1[...]
            for d in range(1, group):
                self.over_plane(d, False).start()

        def step3(self):
            for d in range(1, group):
                self.over_plane(d, True).wait()
            total = self.s1[:, tx, :, pl.ds(pl.multiple_of(an * part, part), part)]
            for d in range(1, group):
                total = total + self.r2[(gid + d) % group]
            self.s2[...] = total
            for d in range(1, n_z):
                self.over_z(d, False).start()

        def step4(self):
            for d in range(1, n_z):
                self.over_z(d, True).wait()
            total = self.s2[z]
            for d in range(1, n_z):
                total = total + self.r3[(z + d) % n_z]
            self.s3[...] = total
            self.g4[pl.ds(gid, 1)] = total[None]
            for d in range(1, group):
                self.over_group(d, False).start()

        def result(self):
            for d in range(1, group):
                self.over_group(d, True).wait()
            return cat([cat([self.g4[a * n_tx + t] for t in range(n_tx)], 0) for a in range(n_an)], 1)

    den_chain, num_chain = Chain(den_refs), Chain(num_refs)

    def some_slots(which, between):
        running = [slot_steps(s) for s in which]
        for n in range(5):
            for steps in running:
                next(steps)
            if n in between:
                between[n]()

    lax.fori_loop(0, slots, extract, 0)
    den_chain.step1()
    some_slots(range(slots // 2), {3: den_chain.step2})
    some_slots(range(slots // 2, slots), {})
    num_chain.step1()
    for d in range(1, group):
        g, where = member(d)
        rdma(pk_own, pk_a.at[g], ksend.at[d], krecv.at[g], where).wait()
    peak = pk_a[0]
    for g in range(1, group):
        peak = jnp.maximum(peak, pk_a[g])
    pk_b[pl.ds(ty, 1)] = peak[None]
    for d in range(1, n_ty):
        rdma(pk_b.at[ty], pk_b.at[ty], lsend.at[d], lrecv.at[ty], {"ty": (ty + d) % n_ty}).start()
    spots = [place(4, s) for s in range(slots)]
    def total_at(start, count, lowest, number):
        def column(n, carry):
            j = lowest + n // 2
            ch = n % 2
            for r in range(0, count, chunk):
                at = start + r if isinstance(start, int) else pl.multiple_of(start + r, 8)
                tot[ch, j, pl.ds(at, chunk), :] = gathered(ch, j, at, chunk, spots)
            return carry

        lax.fori_loop(0, 2 * number, column, 0)

    middle = inner - 2 * margin
    third = middle // 3
    groups = (
        (2 * margin, third), (2 * margin + third, third), (2 * margin + 2 * third, middle - 2 * third),
        (margin, margin), (inner, margin))

    def fold_outer(i):
        start, count = groups[i]
        return rdma(
            region(tot, (outer_at, half), groups[i]), rim_v.at[0, :, pl.ds(start - margin, count)],
            fsend.at[i], frecv.at[i], {"ty": ty + outer_dy})

    def fold_inner():
        return rdma(
            region(tot, (inner_at, half), (margin, inner)), rim_v.at[1], fsend.at[13], frecv.at[13], {"ty": ty + inner_dy})

    def side_of(dx):
        return wide_part(dx, inner, margin)

    def fold_beside(dx, n):
        k = 5 + (dx + 1) // 2 + 6 * n
        start = shared_at if n else pl.multiple_of(half + core * half, 8)
        count = half if n else rows - half
        return rdma(
            region(tot, (start, count), side_of(dx)),
            rim_h.at[(1 - dx) // 2, :, :, pl.ds(pl.multiple_of(start - half, 8), count)],
            fsend.at[k], frecv.at[k], {"tx": tx + dx})

    def fold_corner(dx):
        k = 7 + (dx + 1) // 2
        return rdma(
            region(tot, (outer_at, half), side_of(dx)), rim_h.at[(1 - dx) // 2, :, :, pl.ds(rows, half)],
            fsend.at[k], frecv.at[k], {"tx": tx + dx})

    def fold_pair(dx):
        k = 9 + (dx + 1) // 2
        return rdma(
            region(tot, (inner_at, half), side_of(dx)), pair_h.at[(dx + 1) // 2],
            fsend.at[k], frecv.at[k], {"ty": ty + inner_dy})

    @pl.when(outer_there)
    def _():
        total_at(outer_at, half, *groups[0])
        fold_outer(0).start()

    for dx in (-1, 1):
        @pl.when(beside(dx))
        def _():
            total_at(inner_at, half, *side_of(dx))
            fold_pair(dx).start()
            total_at(outer_at, half, *side_of(dx))
            total_at(half, rows, *side_of(dx))
    num_chain.step2()
    for dx in (-1, 1):
        @pl.when(beside(dx) & outer_there)
        def _():
            fold_corner(dx).start()
    den_chain.step3()
    @pl.when(outer_there)
    def _():
        total_at(outer_at, half, *groups[1])
        fold_outer(1).start()
        for i in (2, 3, 4):
            total_at(outer_at, half, *groups[i])

    total_at(inner_at, half, margin, inner)
    fold_inner().start()
    total_at(half, rows, margin, inner)
    num_chain.step3()

    @pl.when(outer_there)
    def _():
        fold_outer(2).start()

    den_chain.step4()
    for dx in (-1, 1):
        @pl.when(beside(dx))
        def _():
            fold_beside(dx, 0).start()
    p_den = den_chain.result()
    pk_c[pl.ds(ty, 1)] = jnp.broadcast_to(top(p_den), pk_own.shape)[None]
    for d in range(1, n_ty):
        rdma(pk_c.at[ty], pk_c.at[ty], msend.at[d], mrecv.at[ty], {"ty": (ty + d) % n_ty}).start()
    for dx in (-1, 1):
        @pl.when(beside(dx) & outer_there)
        def _():
            fold_corner(-dx).wait_recv()
            start, count = edge_part(dx, inner, margin)
            tot[:, pl.ds(start, count), pl.ds(outer_at, half), :] += rim_h[(dx + 1) // 2, :, :, rows:, :]

    @pl.when(outer_there)
    def _():
        fold_outer(3).start()
        fold_outer(4).start()

    num_chain.step4()
    for dx in (-1, 1):
        @pl.when(beside(dx))
        def _():
            fold_pair(dx).wait()
            tot[:, pl.ds(*side_of(dx)), pl.ds(shared_at, half), :] += pair_h[(dx + 1) // 2]
            fold_beside(dx, 1).start()
    full = num_chain.result()
    p_re, p_im = full[:each], full[each:]

    for dx in (-1, 1):
        @pl.when(beside(dx))
        def _():
            for n in range(2):
                fold_beside(dx, n).wait_send()
                fold_beside(-dx, n).wait_recv()

        @pl.when(beside(dx) & outer_there)
        def _():
            fold_corner(dx).wait_send()

    @pl.when(outer_there)
    def _():
        for i in range(len(groups)):
            fold_outer(i).wait()

    fold_inner().wait()
    for d in range(1, n_ty):
        o = (ty + d) % n_ty
        rdma(pk_b.at[ty], pk_b.at[o], lsend.at[d], lrecv.at[o], {"ty": o}).wait()
    peak = pk_b[0]
    for t in range(1, n_ty):
        peak = jnp.maximum(peak, pk_b[t])
    den[...] = 1.0 / (den[...] + 0.1 * peak[0:1, 0:1])

    for d in range(1, n_ty):
        o = (ty + d) % n_ty
        rdma(pk_c.at[ty], pk_c.at[o], msend.at[d], mrecv.at[o], {"ty": o}).wait()
    peak = pk_c[0]
    for t in range(1, n_ty):
        peak = jnp.maximum(peak, pk_c[t])
    scale = 1.0 / (p_den + 0.1 * peak[0:1, 0:1])
    own_rows = pl.ds(pl.multiple_of(ty * each, each), each)
    out_probe[0] = probe[0, own_rows, :] + p_re * scale
    out_probe[1] = probe[1, own_rows, :] + p_im * scale


def finish_kernel(wide, tot, den, rim_v, rim_h, probe, out, out_probe, held, sems, probe_sem):
    core = lax.axis_index("ty") % 2
    inner, rows, _ = den.shape
    margin, half = rim_h.shape[2], rim_v.shape[3]
    keep_probe = pltpu.make_async_copy(probe, out_probe, probe_sem.at[0])
    keep_probe.start()
    copies = []
    for j in range(inner):
        for ch in range(2):
            for r in range(0, rows, half):
                inside = slice(half + r, half + r + half)
                value = tot[ch, j + margin, inside, :]
                if r < half:
                    value = value + rim_v[core, ch, j, r:r + half, :]
                if r >= rows - half:
                    value = value + rim_v[1 - core, ch, j, r - rows + half:r - rows + 2 * half, :]
                if j < margin:
                    value = value + rim_h[0, ch, j, r:r + half, :]
                if j >= inner - margin:
                    value = value + rim_h[1, ch, j - inner + margin, r:r + half, :]
                held[j, ch, r:r + half, :] = wide[ch, j + margin, inside, :] + value * den[j, r:r + half, :]
        copies.append(pltpu.make_async_copy(held.at[j], out.at[:, :, pl.ds(j * LANES, LANES)], sems.at[j]))
        copies[-1].start()
    for copy in copies:
        copy.wait()
    keep_probe.wait()


def table_values(length):
    half = length // 2
    j, m = np.arange(half), np.arange(half)
    even = 2.0 * math.pi / length * (np.outer(2 * m, j) % length)
    odd = 2.0 * math.pi / length * (np.outer(2 * m + 1, j) % length)
    values = []
    for phase in (even, odd, odd.T):
        values += [np.cos(phase) / math.sqrt(length), np.sin(phase) / math.sqrt(length)]
    high = [value.astype(jnp.bfloat16) for value in values]
    low = [(value - h.astype(np.float64)).astype(jnp.bfloat16) for value, h in zip(values, high)]
    return np.stack(high + low)


def body(shape, object_slices, probe_field, positions, live_slots, photon_counts):
    f32 = jnp.float32
    dma = pltpu.SemaphoreType.DMA
    size = probe_field.shape[1]
    half = size // 2
    tile = object_slices[0]
    _, rows, cols = tile.shape
    spots = positions[0, 0, 0].T
    slots = spots.shape[1]
    inner, margin = cols // LANES, half // LANES
    blocks = inner + 2 * margin
    span = size // LANES + 1
    n_ty, n_tx, n_an = shape["ty"], shape["tx"], shape["angle"]
    n_z, each, group = n_ty // 2, size // n_ty, n_an * n_tx
    part = size // n_an
    vmem = pl.BlockSpec(memory_space=pltpu.VMEM)
    smem = pl.BlockSpec(memory_space=pltpu.SMEM)
    hbm = pl.BlockSpec(memory_space=pltpu.HBM)

    def chain_scratch(height):
        cut = height // n_tx
        return [
            pltpu.VMEM((2, n_z, n_tx, cut, size), f32),
            pltpu.VMEM((n_z, n_tx, cut, size), f32),
            pltpu.VMEM((n_z, n_tx, cut, size), f32),
            pltpu.VMEM((group, n_z, cut, part), f32),
            pltpu.VMEM((n_z, cut, part), f32),
            pltpu.VMEM((n_z, cut, part), f32),
            pltpu.VMEM((cut, part), f32),
            pltpu.VMEM((group, cut, part), f32),
            dma((1,)), dma((1,)), dma((group,)), dma((group,)), dma((n_z,)), dma((n_z,)), dma((group,)), dma((group,)),
        ]

    *parts, new_probe = pl.pallas_call(
        functools.partial(step_kernel, shape),
        out_shape=[pltpu.VMEM(size_of, f32) for size_of in (
            (2, blocks, rows + size, LANES),
            (2, blocks, rows + size, LANES),
            (inner, rows, LANES),
            (2, 2, inner, half, LANES),
            (2, 2, margin, rows + half, LANES),
            (2, each, size),
        )],
        in_specs=[smem, hbm, hbm, hbm, hbm, hbm],
        out_specs=[vmem] * 6,
        scratch_shapes=[
            pltpu.SMEM(spots.shape, jnp.int32),
            pltpu.VMEM((slots, 2, span + 2, rows + 2 * size, LANES), f32),
            pltpu.VMEM((9, 8, LANES), jnp.int32),
            pltpu.SMEM((9, 8, LANES), jnp.int32),
            pltpu.VMEM((2, size, size), f32),
            pltpu.VMEM((slots, size // LANES, size, LANES), jnp.int32),
            pltpu.VMEM((slots, size, size), f32),
            pltpu.VMEM((12, half, half), jnp.bfloat16),
            pltpu.VMEM((2, 4, size, size), jnp.bfloat16),
            pltpu.VMEM((slots, 2, size, size), f32),
            pltpu.VMEM((2, 2, margin, half, LANES), f32),
            pltpu.VMEM((8, LANES), f32),
            pltpu.VMEM((group, 8, LANES), f32),
            pltpu.VMEM((n_ty, 8, LANES), f32),
            pltpu.VMEM((n_ty, 8, LANES), f32),
            dma((12,)), dma((12,)), dma((9,)), dma((9,)),
            dma((14,)), dma((14,)),
            dma((group,)), dma((group,)), dma((n_ty,)), dma((n_ty,)), dma((n_ty,)), dma((n_ty,)),
            dma((4 + size // LANES,)), dma((inner,)),
            *chain_scratch(each), *chain_scratch(2 * each),
        ],
        compiler_params=pltpu.CompilerParams(
            collective_id=0, has_side_effects=True, vmem_limit_bytes=VMEM_LIMIT),
    )(live_slots[0], *[
        pltpu.with_memory_space_constraint(value, pltpu.HBM)
        for value in (spots, tile, probe_field, photon_counts[0, 0, 0], jnp.asarray(table_values(size)))])

    return pl.pallas_call(
        finish_kernel,
        out_shape=(
            jax.ShapeDtypeStruct((2, rows, cols), f32),
            jax.ShapeDtypeStruct((2, each, size), f32),
        ),
        in_specs=[vmem] * 6,
        out_specs=(hbm, hbm),
        scratch_shapes=[pltpu.VMEM((inner, 2, rows, LANES), f32), dma((inner,)), dma((1,))],
        compiler_params=pltpu.CompilerParams(vmem_limit_bytes=FINISH_LIMIT),
    )(*parts, new_probe)


def solution(mesh):
    shape = dict(mesh.shape)

    def step(*args):
        new_tile, new_probe = body(shape, *args)
        return new_tile[None], new_probe

    return jax.shard_map(
        step,
        mesh=mesh,
        in_specs=(
            P("angle", None, "ty", "tx"),
            P(),
            P("angle", "ty", "tx", None, None),
            P("angle", "ty", "tx"),
            P("angle", "ty", "tx", None, None, None),
        ),
        out_specs=(P("angle", None, "ty", "tx"), P(None, "ty", None)),
        check_vma=False,
    )
```

```python
import functools
import math

import jax
import jax.numpy as jnp
import numpy as np
from jax import lax
from jax.experimental import pallas as pl
from jax.experimental.pallas import tpu as pltpu
from jax.sharding import PartitionSpec as P

MESH = pl.DeviceIdType.MESH
LANES = 128
VMEM_LIMIT = 40 * 1024 * 1024
FINISH_LIMIT = 4 * 1024 * 1024
AROUND = tuple((dy, dx) for dy in (-1, 0, 1) for dx in (-1, 0, 1))
BESIDE = tuple(d for d in AROUND if d != (0, 0))
DIAGONALS = tuple(d for d in BESIDE if d[0] and d[1])


def slot_of(dy, dx):
    return (dy + 1) * 3 + dx + 1


def present(dy, dx, shape):
    row = lax.axis_index("ty") + dy
    col = lax.axis_index("tx") + dx
    return (row >= 0) & (row < shape["ty"]) & (col >= 0) & (col < shape["tx"])


def beside_counts(shape):
    found = []
    for axis in ("ty", "tx"):
        at = lax.axis_index(axis)
        found.append(jnp.where(at > 0, 1, 0) + jnp.where(at < shape[axis] - 1, 1, 0))
    return found


def neighbour(dy, dx):
    return {"ty": lax.axis_index("ty") + dy, "tx": lax.axis_index("tx") + dx}


def edge_part(step, size, half):
    return {-1: (half, half), 0: (half, size), 1: (size, half)}[step]


def wide_part(step, size, half):
    return {-1: (0, half), 0: (half, size), 1: (half + size, half)}[step]


def region(ref, rows, blocks):
    return ref.at[:, pl.ds(*blocks), pl.ds(*rows), :]


def split(value):
    high = value.astype(jnp.bfloat16)
    low = (value - high.astype(jnp.float32)).astype(jnp.bfloat16)
    return high, low


def mm(a, b):
    return lax.dot_general(a, b, (((1,), (0,)), ((), ())), preferred_element_type=jnp.float32)


def cat(parts, axis):
    return jnp.concatenate(parts, axis=axis)


def step_kernel(
        shape, live, pos_in, tile_in, probe_in, counts_in, tables_in,
        wide, tot, den, rim_v, rim_h, out_probe,
        pos, dbuf, metas, smetas, probe, counts, amp, tables, mats,
        xbuf, pair_h, pk_own, pk_a, pk_b, pk_c,
        hsend, hrecv, nsend, nrecv, fsend, frecv, ksend, krecv, lsend, lrecv, msend, mrecv, local, local_tile,
        *chain_refs):
    f32 = jnp.float32
    size = probe.shape[1]
    half = size // 2
    slots = counts.shape[0]
    rows, cols = tile_in.shape[1], tile_in.shape[2]
    inner = cols // LANES
    margin = half // LANES
    blocks = inner + 2 * margin
    pieces = size // LANES
    span = pieces + 1
    n_ty, n_tx, n_an = shape["ty"], shape["tx"], shape["angle"]
    ty, tx, an = lax.axis_index("ty"), lax.axis_index("tx"), lax.axis_index("angle")
    core, z = ty % 2, ty // 2
    n_z = n_ty // 2
    group = n_an * n_tx
    gid = an * n_tx + tx
    each = size // n_ty
    part = size // n_an
    den_refs, num_refs = chain_refs[:len(chain_refs) // 2], chain_refs[len(chain_refs) // 2:]
    sums_d, sums_n = den_refs[0], num_refs[0]

    load_pos = pltpu.make_async_copy(pos_in, pos, local.at[3])
    load_pos.start()
    load_tile = [
        pltpu.make_async_copy(
            tile_in.at[:, :, pl.ds(j * LANES, LANES)],
            wide.at[:, margin + j, pl.ds(half, rows), :], local_tile.at[j])
        for j in range(inner)]
    load_probe = pltpu.make_async_copy(probe_in, probe, local.at[0])
    load_counts = [
        pltpu.make_async_copy(counts_in.at[:, :, pl.ds(b * LANES, LANES)], counts.at[:, b], local.at[4 + b])
        for b in range(pieces)]
    load_tables = pltpu.make_async_copy(tables_in, tables, local.at[2])
    for copy in load_tile + load_counts + [load_probe, load_tables]:
        copy.start()

    for k in range(9):
        if k != 4:
            metas[k] = jnp.zeros((8, LANES), jnp.int32)
    barrier = pltpu.get_barrier_semaphore()

    def signal(where):
        pl.semaphore_signal(barrier, inc=1, device_id=where, device_id_type=MESH)

    def member(d):
        a, t = (an + d // n_tx) % n_an, (tx + d % n_tx) % n_tx
        return a * n_tx + t, {"angle": a, "tx": t}

    for d in range(1, n_ty):
        signal({"ty": (ty + d) % n_ty})
    for d in range(1, group):
        signal(member(d)[1])
    for dy, dx in DIAGONALS:
        @pl.when(present(dy, dx, shape))
        def _():
            signal(neighbour(dy, dx))
    outer_dy, inner_dy = 2 * core - 1, 1 - 2 * core
    outer_there = (ty + outer_dy >= 0) & (ty + outer_dy < n_ty)
    outer_at = pl.multiple_of(core * (half + rows), 8)
    shared_at = pl.multiple_of(half + (1 - core) * (rows - half), 8)
    inner_at = pl.multiple_of((1 - core) * (half + rows), 8)

    def beside(dx):
        return (tx + dx >= 0) & (tx + dx < n_tx)

    load_pos.wait()
    lane8 = lax.broadcasted_iota(jnp.int32, (8, LANES), 1)
    line = jnp.zeros((8, LANES), jnp.int32)
    for s in range(slots):
        line = jnp.where(lane8 == s, pos[0, s], line)
        line = jnp.where(lane8 == slots + s, pos[1, s], line)
    line = jnp.where(lane8 == 2 * slots, live[0, 0], line)
    metas[4] = line

    for copy in load_tile:
        copy.wait()
    n_row, n_col = beside_counts(shape)
    pl.semaphore_wait(barrier, n_ty - 1 + group - 1 + n_row * n_col)

    def rdma(src, dst, s_sem, r_sem, where):
        return pltpu.make_async_remote_copy(
            src_ref=src, dst_ref=dst, send_sem=s_sem, recv_sem=r_sem,
            device_id=where, device_id_type=MESH)

    strips = ((margin, margin), (inner, margin), (2 * margin, inner - 2 * margin))
    SIDES = ((-1, 0), (1, 0), (0, -1), (0, 1))

    def halo_v(dy, i):
        src = region(wide, edge_part(dy, rows, half), strips[i])
        dst = region(wide, wide_part(-dy, rows, half), strips[i])
        k = (dy + 1) // 2 * len(strips) + i
        return rdma(src, dst, hsend.at[k], hrecv.at[k], neighbour(dy, 0))

    def halo_h(dx, dy):
        part_rows = wide_part(dy, rows, half)
        src = region(wide, part_rows, edge_part(dx, inner, margin))
        dst = region(wide, part_rows, wide_part(-dx, inner, margin))
        k = 2 * len(strips) + (dx + 1) // 2 * 3 + dy + 1
        return rdma(src, dst, hsend.at[k], hrecv.at[k], neighbour(0, dx))

    def note(dy, dx):
        k = slot_of(dy, dx)
        return rdma(metas.at[4], metas.at[slot_of(-dy, -dx)], nsend.at[k], nrecv.at[k], neighbour(dy, dx))

    order = sorted(BESIDE, key=lambda d: abs(d[1]))
    for dy, dx in order:
        @pl.when(present(dy, dx, shape))
        def _():
            note(dy, dx).start()
    for dy, dx in SIDES:
        @pl.when(present(dy, dx, shape))
        def _():
            if dx == 0:
                halo_v(dy, 0).start()
                halo_v(dy, 1).start()
            else:
                halo_h(dx, 0).start()
    for dy in (-1, 1):
        @pl.when(present(dy, 0, shape))
        def _():
            halo_v(dy, 2).start()

    @pl.when(jnp.logical_not(outer_there))
    def _():
        rim_v[0] = jnp.zeros(rim_v.shape[1:], f32)

    for side, dx in enumerate((-1, 1)):
        @pl.when(jnp.logical_not(beside(dx)))
        def _():
            rim_h[side] = jnp.zeros(rim_h.shape[1:], f32)

    def clear(n, carry):
        s, ch = n // 2, n % 2
        tall = dbuf.shape[3]
        for b in (0, span + 1):
            dbuf[s, ch, b] = jnp.zeros((tall, LANES), f32)
        for b in range(1, span + 1):
            dbuf[s, ch, b, 0:size, :] = jnp.zeros((size, LANES), f32)
            dbuf[s, ch, b, 2 * size:, :] = jnp.zeros((tall - 2 * size, LANES), f32)
        return carry

    lax.fori_loop(0, 2 * slots, clear, 0)
    den[...] = jnp.zeros_like(den)
    sums_d[...] = jnp.zeros_like(sums_d)
    sums_n[...] = jnp.zeros_like(sums_n)

    load_tables.wait()
    for n in range(2):
        ce, se, co, so, cot, sot = [tables[6 * n + i] for i in range(6)]
        for m, (c, up, down) in enumerate(((ce, se, -se), (co, so, -so), (ce, -se, se), (cot, -sot, sot))):
            mats[n, m, 0:half, 0:half] = c
            mats[n, m, 0:half, half:] = up
            mats[n, m, half:, 0:half] = down
            mats[n, m, half:, half:] = c

    for copy in load_counts:
        copy.wait()
    from_lane = lax.broadcasted_iota(jnp.int32, (size, size), 0)
    to_lane = lax.broadcasted_iota(jnp.int32, (size, size), 1)
    wanted = jnp.where(to_lane < half, 2 * to_lane, 2 * (to_lane - half) + 1)
    shuffle = jnp.where(from_lane == wanted, 1.0, 0.0).astype(jnp.bfloat16)
    shuffle2 = cat([shuffle, shuffle], 0)

    def amplitude(s, carry):
        seen = cat([
            cat([counts[s, b, pl.ds(n, half, stride=2), :] for b in range(pieces)], 1) for n in range(2)], 0).astype(f32)
        amp[s] = 0.05 * jnp.sqrt(mm(cat(list(split(seen)), 1), shuffle2))
        return carry

    lax.fori_loop(0, slots, amplitude, 0)

    load_probe.wait()
    for dy, dx in order:
        @pl.when(present(dy, dx, shape))
        def _():
            note(dy, dx).wait_send()
            note(-dy, -dx).wait_recv()
    for dy in (-1, 1):
        @pl.when(present(dy, 0, shape))
        def _():
            halo_v(-dy, 0).wait_recv()
            halo_v(-dy, 1).wait_recv()
    for dy, dx in DIAGONALS:
        @pl.when(present(dy, dx, shape))
        def _():
            halo_h(dx, dy).start()
    to_scalar = pltpu.make_async_copy(metas, smetas, local.at[3])
    to_scalar.start()
    to_scalar.wait()

    lane = lax.broadcasted_iota(jnp.int32, (size, LANES), 1)

    def spread(piece, shift):
        moved = [pltpu.roll(piece[:, b * LANES:(b + 1) * LANES], shift, axis=1) for b in range(pieces)]
        low = lane[:piece.shape[0]] < shift
        found = [jnp.where(low, 0.0, moved[0])]
        for b in range(1, pieces):
            found.append(jnp.where(low, moved[b - 1], moved[b]))
        found.append(jnp.where(low, moved[-1], 0.0))
        return found

    def spot(k, s):
        return smetas[k, 0, s] - ty * rows + half, smetas[k, 0, slots + s] - tx * cols + half

    far = 64 * LANES

    def place(k, s):
        dy, dx = k // 3 - 1, k % 3 - 1
        row, at = spot(k, s)
        row = jnp.clip(row, dy * rows, dy * rows + rows - 1)
        at = jnp.clip(at, dx * cols, dx * cols + cols - 1)
        first = (at + far * LANES) // LANES - far
        return row, first, (at + far * LANES) % LANES

    power = probe[0] * probe[0] + probe[1] * probe[1]
    base = size

    def gathered(ch, j, start, count, spots):
        total = None
        for s, (row, first, _) in enumerate(spots):
            b = jnp.clip(j - first + 1, 0, span + 1)
            value = dbuf[s, ch, b, pl.ds(start - row + base, count), :]
            total = value if total is None else total + value
        return total

    chunk = half
    for k, (dy, dx) in enumerate(AROUND):
        there = present(dy, dx, shape)
        spots = [place(k, s) for s in range(slots)]

        part_rows = {-1: (half, size), 0: (0, size), 1: (0, half)}[dy]
        for s in range(slots):
            used = there & (s < smetas[k, 0, 2 * slots])
            piece = jnp.where(used, power[part_rows[0]:part_rows[1]], 0.0)
            for b, value in enumerate(spread(piece, spots[s][2])):
                dbuf[s, 0, 1 + b, size + part_rows[0]:size + part_rows[1], :] = value
        tall = range(0, rows, chunk) if dy == 0 else (range(0, half, chunk) if dy < 0 else range(rows - half, rows, chunk))
        if dx == 0:
            def column(j, carry):
                for r in tall:
                    den[j, r:r + chunk, :] += gathered(0, j + margin, half + r, chunk, spots)
                return carry

            lax.fori_loop(0, inner, column, 0)
        else:
            for j in range(margin) if dx < 0 else range(inner - margin, inner):
                for r in tall:
                    den[j, r:r + chunk, :] += gathered(0, j + margin, half + r, chunk, spots)

    def top(value):
        return jnp.max(jnp.max(value, axis=0, keepdims=True), axis=1, keepdims=True)

    pk_own[...] = jnp.broadcast_to(top(jnp.max(den[...], axis=0)), pk_own.shape)
    pk_a[pl.ds(gid, 1)] = pk_own[...][None]
    for d in range(1, group):
        g, where = member(d)
        rdma(pk_own, pk_a.at[gid], ksend.at[d], krecv.at[gid], where).start()

    for dy, dx in SIDES:
        @pl.when(present(dy, dx, shape))
        def _():
            if dx == 0:
                for i in range(len(strips)):
                    halo_v(dy, i).wait_send()
                halo_v(-dy, 2).wait_recv()
            else:
                halo_h(dx, 0).wait_send()
                halo_h(-dx, 0).wait_recv()
    for dy, dx in DIAGONALS:
        @pl.when(present(dy, dx, shape))
        def _():
            halo_h(dx, dy).wait_send()
            halo_h(-dx, dy).wait_recv()

    def matrix(m, axis):
        return cat([mats[0, m], mats[0, m], mats[1, m]], axis)

    def from_left(m, re, im):
        high, low = split(cat([re, im], 0))
        found = mm(matrix(m, 1), cat([high, low, high], 0))
        return found[:half], found[half:]

    def from_right(m, re, im):
        high, low = split(cat([re, im], 1))
        found = mm(cat([high, low, high], 1), matrix(m, 0))
        return found[:, :half], found[:, half:]

    def add_to(total, values):
        cut = total.shape[3]
        length = min(cut, each)
        for t in range(n_ty):
            for ch, value in enumerate(values):
                for i in range(0, each, length):
                    at = ch * each + i
                    total[t % 2, t // 2, at // cut, at % cut:at % cut + length, :] += (
                        value[t * each + i:t * each + i + length, :])

    def extract(s, carry):
        row, first, shift = place(4, s)
        used = s < smetas[4, 0, 2 * slots]
        back = (LANES - shift) % LANES
        keep = lane < LANES - shift
        found = []
        for ch in range(2):
            moved = [
                pltpu.roll(wide[ch, first + b, pl.ds(row, size), :], back, axis=1)
                for b in range(span)]
            found.append(cat([jnp.where(keep, moved[b], moved[b + 1]) for b in range(pieces)], 1))
            xbuf[s, ch] = found[ch]
        add_to(sums_d, (jnp.where(used, found[0] * found[0] + found[1] * found[1], 0.0),))
        return carry

    def slot_steps(s):
        shift = place(4, s)[2]
        used = s < smetas[4, 0, 2 * slots]

        def psi():
            x_re, x_im = xbuf[s, 0], xbuf[s, 1]
            q_re, q_im = probe[0], probe[1]
            return q_re * x_re - q_im * x_im, q_re * x_im + q_im * x_re

        p_re, p_im = psi()
        a = from_left(0, p_re[:half] + p_re[half:], p_im[:half] + p_im[half:])
        b = from_left(1, p_re[:half] - p_re[half:], p_im[:half] - p_im[half:])
        yield
        y_re, y_im = cat([a[0], b[0]], 0), cat([a[1], b[1]], 0)
        a = from_right(2, y_re[:, :half] + y_re[:, half:], y_im[:, :half] + y_im[:, half:])
        b = from_right(3, y_re[:, :half] - y_re[:, half:], y_im[:, :half] - y_im[:, half:])
        yield
        f_re, f_im = cat([a[0], b[0]], 1), cat([a[1], b[1]], 1)
        factor = amp[s] * lax.rsqrt(jnp.maximum(f_re * f_re + f_im * f_im, 0.0625))
        g_re, g_im = f_re * factor, f_im * factor
        a = from_left(2, g_re[:half], g_im[:half])
        b = from_left(3, g_re[half:], g_im[half:])
        yield
        y_re, y_im = cat([a[0] + b[0], a[0] - b[0]], 0), cat([a[1] + b[1], a[1] - b[1]], 0)
        a = from_right(0, y_re[:, :half], y_im[:, :half])
        b = from_right(1, y_re[:, half:], y_im[:, half:])
        yield
        p_re, p_im = psi()
        b_re, b_im = cat([a[0] + b[0], a[0] - b[0]], 1), cat([a[1] + b[1], a[1] - b[1]], 1)
        d_re, d_im = jnp.where(used, b_re - p_re, 0.0), jnp.where(used, b_im - p_im, 0.0)
        x_re, x_im = xbuf[s, 0], xbuf[s, 1]
        q_re, q_im = probe[0], probe[1]
        for ch, value in enumerate((q_re * d_re + q_im * d_im, q_re * d_im - q_im * d_re)):
            for i, moved in enumerate(spread(value, shift)):
                dbuf[s, ch, 1 + i, size:2 * size, :] = moved
        add_to(sums_n, (x_re * d_re + x_im * d_im, x_re * d_im - x_im * d_re))
        yield

    class Chain:
        def __init__(self, refs):
            (self.sums, self.r1, self.s1, self.r2, self.s2, self.r3, self.s3, self.g4,
             self.send1, self.recv1, self.send2, self.recv2, self.send3, self.recv3, self.send4, self.recv4) = refs

        def pair(self):
            return rdma(self.sums.at[1 - core], self.r1, self.send1.at[0], self.recv1.at[0], {"ty": ty + 1 - 2 * core})

        def over_plane(self, d, get):
            g, where = member(d)
            at = g if get else gid
            lanes = pl.ds(pl.multiple_of(g // n_tx * part, part), part)
            return rdma(
                self.s1.at[:, g % n_tx, :, lanes], self.r2.at[at], self.send2.at[d], self.recv2.at[at], where)

        def over_z(self, d, get):
            o = (z + d) % n_z
            at = o if get else z
            return rdma(self.s2.at[o], self.r3.at[at], self.send3.at[d], self.recv3.at[at], {"ty": o * 2 + core})

        def over_group(self, d, get):
            g, where = member(d)
            at = g if get else gid
            return rdma(self.s3, self.g4.at[at], self.send4.at[d], self.recv4.at[at], where)

        def step1(self):
            self.pair().start()

        def step2(self):
            self.pair().wait()
            self.s1[...] = self.sums[core] + self.r1[...]
            for d in reversed(range(1, group)):
                self.over_plane(d, False).start()

        def step3(self):
            for d in range(1, group):
                self.over_plane(d, True).wait()
            total = self.s1[:, tx, :, pl.ds(pl.multiple_of(an * part, part), part)]
            for d in range(1, group):
                total = total + self.r2[(gid + d) % group]
            self.s2[...] = total
            for d in range(1, n_z):
                self.over_z(d, False).start()

        def step4(self):
            for d in range(1, n_z):
                self.over_z(d, True).wait()
            total = self.s2[z]
            for d in range(1, n_z):
                total = total + self.r3[(z + d) % n_z]
            self.s3[...] = total
            self.g4[pl.ds(gid, 1)] = total[None]
            for d in reversed(range(1, group)):
                self.over_group(d, False).start()

        def result(self):
            for d in range(1, group):
                self.over_group(d, True).wait()
            return cat([cat([self.g4[a * n_tx + t] for t in range(n_tx)], 0) for a in range(n_an)], 1)

    den_chain, num_chain = Chain(den_refs), Chain(num_refs)

    def some_slots(which, between):
        running = [slot_steps(s) for s in which]
        for n in range(5):
            for steps in running:
                next(steps)
            if n in between:
                between[n]()

    lax.fori_loop(0, slots, extract, 0)
    den_chain.step1()
    some_slots(range(slots // 2), {3: den_chain.step2})
    some_slots(range(slots // 2, slots), {})
    num_chain.step1()
    for d in range(1, group):
        g, where = member(d)
        rdma(pk_own, pk_a.at[g], ksend.at[d], krecv.at[g], where).wait()
    peak = pk_a[0]
    for g in range(1, group):
        peak = jnp.maximum(peak, pk_a[g])
    pk_b[pl.ds(ty, 1)] = peak[None]
    for d in range(1, n_ty):
        rdma(pk_b.at[ty], pk_b.at[ty], lsend.at[d], lrecv.at[ty], {"ty": (ty + d) % n_ty}).start()
    spots = [place(4, s) for s in range(slots)]
    def total_at(start, count, lowest, number):
        def column(n, carry):
            j = lowest + n // 2
            ch = n % 2
            for r in range(0, count, chunk):
                at = start + r if isinstance(start, int) else pl.multiple_of(start + r, 8)
                tot[ch, j, pl.ds(at, chunk), :] = gathered(ch, j, at, chunk, spots)
            return carry

        lax.fori_loop(0, 2 * number, column, 0)

    middle = inner - 2 * margin
    third = middle // 3
    groups = (
        (2 * margin, third), (2 * margin + third, third), (2 * margin + 2 * third, middle - 2 * third),
        (margin, margin), (inner, margin))

    def fold_outer(i):
        start, count = groups[i]
        return rdma(
            region(tot, (outer_at, half), groups[i]), rim_v.at[0, :, pl.ds(start - margin, count)],
            fsend.at[i], frecv.at[i], {"ty": ty + outer_dy})

    def fold_inner():
        return rdma(
            region(tot, (inner_at, half), (margin, inner)), rim_v.at[1], fsend.at[13], frecv.at[13], {"ty": ty + inner_dy})

    def side_of(dx):
        return wide_part(dx, inner, margin)

    def fold_beside(dx, n):
        k = 5 + (dx + 1) // 2 + 6 * n
        start = shared_at if n else pl.multiple_of(half + core * half, 8)
        count = half if n else rows - half
        return rdma(
            region(tot, (start, count), side_of(dx)),
            rim_h.at[(1 - dx) // 2, :, :, pl.ds(pl.multiple_of(start - half, 8), count)],
            fsend.at[k], frecv.at[k], {"tx": tx + dx})

    def fold_corner(dx):
        k = 7 + (dx + 1) // 2
        return rdma(
            region(tot, (outer_at, half), side_of(dx)), rim_h.at[(1 - dx) // 2, :, :, pl.ds(rows, half)],
            fsend.at[k], frecv.at[k], {"tx": tx + dx})

    def fold_pair(dx):
        k = 9 + (dx + 1) // 2
        return rdma(
            region(tot, (inner_at, half), side_of(dx)), pair_h.at[(dx + 1) // 2],
            fsend.at[k], frecv.at[k], {"ty": ty + inner_dy})

    @pl.when(outer_there)
    def _():
        total_at(outer_at, half, *groups[0])
        fold_outer(0).start()

    for dx in (-1, 1):
        @pl.when(beside(dx))
        def _():
            total_at(inner_at, half, *side_of(dx))
            fold_pair(dx).start()
            total_at(outer_at, half, *side_of(dx))
            total_at(half, rows, *side_of(dx))
    num_chain.step2()
    for dx in (-1, 1):
        @pl.when(beside(dx) & outer_there)
        def _():
            fold_corner(dx).start()
    den_chain.step3()
    @pl.when(outer_there)
    def _():
        total_at(outer_at, half, *groups[1])
        fold_outer(1).start()
        for i in (2, 3, 4):
            total_at(outer_at, half, *groups[i])

    total_at(inner_at, half, margin, inner)
    fold_inner().start()
    total_at(half, rows, margin, inner)
    num_chain.step3()

    @pl.when(outer_there)
    def _():
        fold_outer(2).start()

    den_chain.step4()
    for dx in (-1, 1):
        @pl.when(beside(dx))
        def _():
            fold_beside(dx, 0).start()
    p_den = den_chain.result()
    pk_c[pl.ds(ty, 1)] = jnp.broadcast_to(top(p_den), pk_own.shape)[None]
    for d in range(1, n_ty):
        rdma(pk_c.at[ty], pk_c.at[ty], msend.at[d], mrecv.at[ty], {"ty": (ty + d) % n_ty}).start()
    for dx in (-1, 1):
        @pl.when(beside(dx) & outer_there)
        def _():
            fold_corner(-dx).wait_recv()
            start, count = edge_part(dx, inner, margin)
            tot[:, pl.ds(start, count), pl.ds(outer_at, half), :] += rim_h[(dx + 1) // 2, :, :, rows:, :]

    @pl.when(outer_there)
    def _():
        fold_outer(3).start()
        fold_outer(4).start()

    num_chain.step4()
    for dx in (-1, 1):
        @pl.when(beside(dx))
        def _():
            fold_pair(dx).wait()
            tot[:, pl.ds(*side_of(dx)), pl.ds(shared_at, half), :] += pair_h[(dx + 1) // 2]
            fold_beside(dx, 1).start()
    for d in range(1, n_ty):
        o = (ty + d) % n_ty
        rdma(pk_b.at[ty], pk_b.at[o], lsend.at[d], lrecv.at[o], {"ty": o}).wait()
    peak = pk_b[0]
    for t in range(1, n_ty):
        peak = jnp.maximum(peak, pk_b[t])
    den[...] = 1.0 / (den[...] + 0.1 * peak[0:1, 0:1])
    full = num_chain.result()
    p_re, p_im = full[:each], full[each:]

    for dx in (-1, 1):
        @pl.when(beside(dx))
        def _():
            for n in range(2):
                fold_beside(dx, n).wait_send()
                fold_beside(-dx, n).wait_recv()

        @pl.when(beside(dx) & outer_there)
        def _():
            fold_corner(dx).wait_send()

    @pl.when(outer_there)
    def _():
        for i in range(len(groups)):
            fold_outer(i).wait()

    fold_inner().wait()

    for d in range(1, n_ty):
        o = (ty + d) % n_ty
        rdma(pk_c.at[ty], pk_c.at[o], msend.at[d], mrecv.at[o], {"ty": o}).wait()
    peak = pk_c[0]
    for t in range(1, n_ty):
        peak = jnp.maximum(peak, pk_c[t])
    scale = 1.0 / (p_den + 0.1 * peak[0:1, 0:1])
    own_rows = pl.ds(pl.multiple_of(ty * each, each), each)
    out_probe[0] = probe[0, own_rows, :] + p_re * scale
    out_probe[1] = probe[1, own_rows, :] + p_im * scale


def finish_kernel(wide, tot, den, rim_v, rim_h, probe, out, out_probe, held, sems, probe_sem):
    core = lax.axis_index("ty") % 2
    inner, rows, _ = den.shape
    margin, half = rim_h.shape[2], rim_v.shape[3]
    keep_probe = pltpu.make_async_copy(probe, out_probe, probe_sem.at[0])
    keep_probe.start()
    copies = []
    for j in range(inner):
        for ch in range(2):
            for r in range(0, rows, half):
                inside = slice(half + r, half + r + half)
                value = tot[ch, j + margin, inside, :]
                if r < half:
                    value = value + rim_v[core, ch, j, r:r + half, :]
                if r >= rows - half:
                    value = value + rim_v[1 - core, ch, j, r - rows + half:r - rows + 2 * half, :]
                if j < margin:
                    value = value + rim_h[0, ch, j, r:r + half, :]
                if j >= inner - margin:
                    value = value + rim_h[1, ch, j - inner + margin, r:r + half, :]
                held[j, ch, r:r + half, :] = wide[ch, j + margin, inside, :] + value * den[j, r:r + half, :]
        copies.append(pltpu.make_async_copy(held.at[j], out.at[:, :, pl.ds(j * LANES, LANES)], sems.at[j]))
        copies[-1].start()
    for copy in copies:
        copy.wait()
    keep_probe.wait()


def table_values(length):
    half = length // 2
    j, m = np.arange(half), np.arange(half)
    even = 2.0 * math.pi / length * (np.outer(2 * m, j) % length)
    odd = 2.0 * math.pi / length * (np.outer(2 * m + 1, j) % length)
    values = []
    for phase in (even, odd, odd.T):
        values += [np.cos(phase) / math.sqrt(length), np.sin(phase) / math.sqrt(length)]
    high = [value.astype(jnp.bfloat16) for value in values]
    low = [(value - h.astype(np.float64)).astype(jnp.bfloat16) for value, h in zip(values, high)]
    return np.stack(high + low)


def body(shape, object_slices, probe_field, positions, live_slots, photon_counts):
    f32 = jnp.float32
    dma = pltpu.SemaphoreType.DMA
    size = probe_field.shape[1]
    half = size // 2
    tile = object_slices[0]
    _, rows, cols = tile.shape
    spots = positions[0, 0, 0].T
    slots = spots.shape[1]
    inner, margin = cols // LANES, half // LANES
    blocks = inner + 2 * margin
    span = size // LANES + 1
    n_ty, n_tx, n_an = shape["ty"], shape["tx"], shape["angle"]
    n_z, each, group = n_ty // 2, size // n_ty, n_an * n_tx
    part = size // n_an
    vmem = pl.BlockSpec(memory_space=pltpu.VMEM)
    smem = pl.BlockSpec(memory_space=pltpu.SMEM)
    hbm = pl.BlockSpec(memory_space=pltpu.HBM)

    def chain_scratch(height):
        cut = height // n_tx
        return [
            pltpu.VMEM((2, n_z, n_tx, cut, size), f32),
            pltpu.VMEM((n_z, n_tx, cut, size), f32),
            pltpu.VMEM((n_z, n_tx, cut, size), f32),
            pltpu.VMEM((group, n_z, cut, part), f32),
            pltpu.VMEM((n_z, cut, part), f32),
            pltpu.VMEM((n_z, cut, part), f32),
            pltpu.VMEM((cut, part), f32),
            pltpu.VMEM((group, cut, part), f32),
            dma((1,)), dma((1,)), dma((group,)), dma((group,)), dma((n_z,)), dma((n_z,)), dma((group,)), dma((group,)),
        ]

    *parts, new_probe = pl.pallas_call(
        functools.partial(step_kernel, shape),
        out_shape=[pltpu.VMEM(size_of, f32) for size_of in (
            (2, blocks, rows + size, LANES),
            (2, blocks, rows + size, LANES),
            (inner, rows, LANES),
            (2, 2, inner, half, LANES),
            (2, 2, margin, rows + half, LANES),
            (2, each, size),
        )],
        in_specs=[smem, hbm, hbm, hbm, hbm, hbm],
        out_specs=[vmem] * 6,
        scratch_shapes=[
            pltpu.SMEM(spots.shape, jnp.int32),
            pltpu.VMEM((slots, 2, span + 2, rows + 2 * size, LANES), f32),
            pltpu.VMEM((9, 8, LANES), jnp.int32),
            pltpu.SMEM((9, 8, LANES), jnp.int32),
            pltpu.VMEM((2, size, size), f32),
            pltpu.VMEM((slots, size // LANES, size, LANES), jnp.int32),
            pltpu.VMEM((slots, size, size), f32),
            pltpu.VMEM((12, half, half), jnp.bfloat16),
            pltpu.VMEM((2, 4, size, size), jnp.bfloat16),
            pltpu.VMEM((slots, 2, size, size), f32),
            pltpu.VMEM((2, 2, margin, half, LANES), f32),
            pltpu.VMEM((8, LANES), f32),
            pltpu.VMEM((group, 8, LANES), f32),
            pltpu.VMEM((n_ty, 8, LANES), f32),
            pltpu.VMEM((n_ty, 8, LANES), f32),
            dma((12,)), dma((12,)), dma((9,)), dma((9,)),
            dma((14,)), dma((14,)),
            dma((group,)), dma((group,)), dma((n_ty,)), dma((n_ty,)), dma((n_ty,)), dma((n_ty,)),
            dma((4 + size // LANES,)), dma((inner,)),
            *chain_scratch(each), *chain_scratch(2 * each),
        ],
        compiler_params=pltpu.CompilerParams(
            collective_id=0, has_side_effects=True, vmem_limit_bytes=VMEM_LIMIT),
    )(live_slots[0], *[
        pltpu.with_memory_space_constraint(value, pltpu.HBM)
        for value in (spots, tile, probe_field, photon_counts[0, 0, 0], jnp.asarray(table_values(size)))])

    return pl.pallas_call(
        finish_kernel,
        out_shape=(
            jax.ShapeDtypeStruct((2, rows, cols), f32),
            jax.ShapeDtypeStruct((2, each, size), f32),
        ),
        in_specs=[vmem] * 6,
        out_specs=(hbm, hbm),
        scratch_shapes=[pltpu.VMEM((inner, 2, rows, LANES), f32), dma((inner,)), dma((1,))],
        compiler_params=pltpu.CompilerParams(vmem_limit_bytes=FINISH_LIMIT),
    )(*parts, new_probe)


def solution(mesh):
    shape = dict(mesh.shape)

    def step(*args):
        new_tile, new_probe = body(shape, *args)
        return new_tile[None], new_probe

    return jax.shard_map(
        step,
        mesh=mesh,
        in_specs=(
            P("angle", None, "ty", "tx"),
            P(),
            P("angle", "ty", "tx", None, None),
            P("angle", "ty", "tx"),
            P("angle", "ty", "tx", None, None, None),
        ),
        out_specs=(P("angle", None, "ty", "tx"), P(None, "ty", None)),
        check_vma=False,
    )
```
